32 devices in a mesh: scen: 8 (over y, x, core), base: 4 (over z).
Axes of the slice: x: 2, y: 2, z: 4, core: 2. Of those that a mesh axis runs over, the one named last changes fastest.
Arguments:
- right_sides: float32 [32, 8192], P(None, 'scen'), may hold values from -6 to 6
- base_hessian: float32 [8192], P('scen'), may hold values from 0.05 to 1
- sensitivity: float32 [16, 8192, 128], P('base', 'scen'), may hold values from -0.1875 to 0.1875
- weights: float32 [16, 128], P('base'), may hold values from 0.1 to 10
- outage_factors: float32 [16, 128], P('base'), may hold values from -1 to 1
- outaged: int32 [16], P('base'), may hold values from 0 to 127
Outputs:
- step: float32 [32, 8192], P(None, 'scen')
- flow_step: float32 [16, 32, 128], P('base')
The draws below stay inside these ranges and needn't reach their ends.
All inputs are finite; a program needn't handle non-finite values.
Results may differ from the reference program's by a relative error of at most 0.0003.
Values sent between devices are 32-bit elements; how exact they have to be, the bound alone decides.
No kernel may reach another device: no remote copies, remote signals or barrier semaphores. Data moves between devices by JAX's collectives and lax.ppermute only.
A program may use at most 64 MiB of HBM per device.

```python
import math
import jax
import jax.numpy as jnp
from jax import lax

NVAR = 8192
LINES = 128
RHS = 32
ITERS = 5
CONT = 16


def touch_ends(values, stream_key, smallest, largest):
    longest = values.shape.index(max(values.shape))
    spots = []
    for shift in (0, 1):
        where = [jax.random.randint(jax.random.fold_in(stream_key, axis), (), 0, length) for axis, length in enumerate(values.shape)]
        where[longest] = (where[longest] + shift) % values.shape[longest]
        spots.append(tuple(where))
    return values.at[spots[0]].set(smallest).at[spots[1]].set(largest)


def with_spikes(drawn, rng, source, target, parts, factor):
    owner, partner = [(jnp.arange(drawn.shape[axis_at]) // (drawn.shape[axis_at] // parts)).reshape([-1 if axis == axis_at else 1 for axis in range(drawn.ndim)]) for axis_at in (source, target)]
    chosen = jax.random.permutation(rng, parts)[partner]
    strong = (owner == chosen) | (owner == (partner + parts // 2) % parts)
    return jnp.where(strong, factor * drawn, drawn)


def levels(own_key, shape, shards, smallest, largest):
    gain, own = 1.0, jax.random.fold_in(own_key, 6)
    for dim, parts in shards:
        heights = jnp.exp(jax.random.uniform(jax.random.fold_in(own, dim), (parts,), jnp.float32, smallest / len(shards), largest / len(shards)))
        gain = gain * jnp.repeat(heights, shape[dim] // parts).reshape([-1 if axis == dim else 1 for axis in range(len(shape))])
    return gain


def noise(key, extent, deviation, reach, cuts=(), held_as=jnp.bfloat16):
    gain = levels(key, extent, cuts, -0.22, 0.18) if cuts else 1.0
    result = jax.random.normal(key, extent, jnp.float32) * deviation * gain
    return jnp.minimum(jnp.maximum(result, -reach), reach).astype(held_as)


def heavy_noise(own_key, dims, scale, bound, shards, heavy, kind=jnp.bfloat16):
    result = scale * jax.random.normal(own_key, dims, jnp.float32)
    if shards:
        result = result * levels(own_key, dims, shards, -0.22, 0.18)
    return jnp.clip(with_spikes(result, jax.random.fold_in(own_key, 3), *heavy), -bound, bound).astype(kind)


def setup_inputs(seed: int = 0) -> dict:
    seeds = jax.random.split(jax.random.key(seed), 7)
    return {
        "right_sides": noise(seeds[0], (RHS, NVAR), 1.0, 6.0, ((1, 8),), jnp.float32),
        "base_hessian": jnp.clip(jnp.exp(math.log(1.0) - 2.9957323 * jax.random.uniform(seeds[1], (NVAR,), jnp.float32) ** levels(seeds[1], (NVAR,), ((0, 8),), -0.2, 0.2)), 0.05, 1.0),
        "sensitivity": heavy_noise(seeds[2], (CONT, NVAR, LINES), (CONT * LINES) ** -0.5, 0.1875, ((0, 4), (1, 8)), (0, 1, 8, 2.0), jnp.float32),
        "weights": jnp.clip(jnp.exp(math.log(10.0) - 4.6051702 * jax.random.uniform(seeds[3], (CONT, LINES), jnp.float32) ** levels(seeds[3], (CONT, LINES), ((0, 4),), -0.2, 0.2)), 0.1, 10.0),
        "outage_factors": jnp.clip(jax.random.uniform(seeds[4], (CONT, LINES), jnp.float32, -1.0, 1.0) * levels(seeds[4], (CONT, LINES), ((0, 4),), -0.4, 0.0), -1.0, 1.0),
        "outaged": touch_ends(jax.random.randint(seeds[5], (CONT,), 0, LINES), jax.random.fold_in(seeds[5], 1), 0, LINES - 1).astype(jnp.int32),
    }


HIGHEST_PREC = lax.Precision.HIGHEST


def contingency_terms(flows_sum, weights, selector, factors):
    outaged_flow = jnp.sum(flows_sum * selector[:, None, :], axis=2, keepdims=True)
    post_flows = flows_sum + factors[:, None, :] * outaged_flow
    weighted = weights[:, None, :] * post_flows
    outaged_sum = jnp.sum(factors[:, None, :] * weighted, axis=2, keepdims=True)
    spread_back = weighted + selector[:, None, :] * outaged_sum
    return post_flows, weighted, spread_back


def reference(right_sides, base_hessian, sensitivity, weights, outage_factors, outaged):
    chosen = lax.broadcasted_iota(jnp.int32, weights.shape, 1) == outaged[:, None].astype(jnp.int32)
    selector = chosen.astype(weights.dtype)
    factors = jnp.where(chosen, -1.0, outage_factors).astype(weights.dtype)

    def apply_schur(direction):
        flows_sum = jnp.einsum('knm,rn->krm', sensitivity, direction, precision=HIGHEST_PREC)
        post_flows, weighted, spread_back = contingency_terms(flows_sum, weights, selector, factors)
        product = jnp.einsum('knm,krm->rn', sensitivity, spread_back, precision=HIGHEST_PREC)
        return product + base_hessian[None, :] * direction, weighted

    solution = jnp.zeros_like(right_sides)
    residual = right_sides
    direction = right_sides
    norm_now = jnp.sum(residual * residual, axis=1)
    for iteration in range(ITERS):
        product, unused = apply_schur(direction)
        step_len = norm_now / jnp.sum(direction * product, axis=1)
        solution = solution + step_len[:, None] * direction
        residual = residual - step_len[:, None] * product
        norm_next = jnp.sum(residual * residual, axis=1)
        direction = residual + (norm_next / norm_now)[:, None] * direction
        norm_now = norm_next
    flows_sum = jnp.einsum('knm,rn->krm', sensitivity, solution, precision=HIGHEST_PREC)
    post_flows, weighted, spread_back = contingency_terms(flows_sum, weights, selector, factors)
    return solution, weighted
```

```python
import functools

import jax
import jax.numpy as jnp
from jax import lax
from jax.experimental import pallas as pl
from jax.experimental.pallas import tpu as pltpu
from jax.sharding import PartitionSpec as P

ITERS = 5
LANE = 128
F32 = jnp.float32
BF16 = jnp.bfloat16
VM = pl.BlockSpec(memory_space=pltpu.VMEM)
SM = pl.BlockSpec(memory_space=pltpu.SMEM)
PARAMS = pltpu.CompilerParams(vmem_limit_bytes=24 * 1024 * 1024)


def call(body, out_shape, name, *args, scalars=0):
    specs = [VM] * (len(args) - scalars) + [SM] * scalars
    many = isinstance(out_shape, (list, tuple))
    return pl.pallas_call(
        body,
        out_shape=out_shape,
        in_specs=specs,
        out_specs=[VM] * len(out_shape) if many else VM,
        compiler_params=PARAMS,
        name=name,
    )(*args)


def struct(shape, dtype=F32):
    return jax.ShapeDtypeStruct(shape, dtype)


def split(value):
    high = value.astype(BF16)
    low = (value - high.astype(F32)).astype(BF16)
    return high, low


def stacked(value):
    high, low = split(value)
    return jnp.concatenate([high, low], axis=0)


def lane_index(shape):
    return lax.broadcasted_iota(jnp.int32, shape, 1)


def convert_body(a_ref, high_ref, low_ref):
    for k in range(a_ref.shape[0]):
        high, low = split(a_ref[k])
        high_ref[:, k * LANE:(k + 1) * LANE] = high
        low_ref[:, k * LANE:(k + 1) * LANE] = low


def convert(a):
    k, n, m = a.shape
    shape = struct((n, k * m), BF16)
    return call(convert_body, [shape, shape], "convert", a)


def dot(lhs, rhs, rhs_dim):
    return lax.dot_general(lhs, rhs, (((1,), (rhs_dim,)), ((), ())), preferred_element_type=F32)


def to_lines(vector, mats):
    rows, n = vector.shape[0], vector.shape[1] // 2
    total = None
    for half in range(2):
        pair = stacked(vector[:, half * n:(half + 1) * n])
        for part in range(2):
            out = dot(pair, mats[2 * half + part][...], 0)
            total = out if total is None else total + out
    return total[:rows] + total[rows:]


def from_lines(lines, mats):
    rows = lines.shape[0]
    pair = stacked(lines)
    halves = []
    for half in range(2):
        out = dot(pair, mats[2 * half][...], 1) + dot(pair, mats[2 * half + 1][...], 1)
        halves.append(out[:rows] + out[rows:])
    return halves


def store_flows(vector, hess, previous, mats, payload_ref):
    rows = vector.shape[0]
    lines = to_lines(vector, mats)
    conts = lines.shape[1] // LANE
    for k in range(conts):
        payload_ref[k * rows:(k + 1) * rows, :] = lines[:, k * LANE:(k + 1) * LANE]
    scaled = hess * vector
    first = jnp.sum(vector * vector, axis=1, keepdims=True)
    second = jnp.sum(scaled * vector, axis=1, keepdims=True)
    lane = lane_index((rows, LANE))
    packed = jnp.where(lane == 0, first, 0.0) + jnp.where(lane == 1, second, 0.0)
    if previous is not None:
        third = jnp.sum(scaled * previous, axis=1, keepdims=True)
        packed = packed + jnp.where(lane == 2, third, 0.0)
    payload_ref[conts * rows:(conts + 1) * rows, :] = packed


def first_body(r_ref, hess_ref, a0, a1, a2, a3, payload_ref):
    store_flows(r_ref[...], hess_ref[...], None, (a0, a1, a2, a3), payload_ref)


def step_body(za_ref, zb_ref, r_ref, p_ref, x_ref, sc_ref, hess_ref, a0, a1, a2, a3,
              payload_ref, rn_ref, pn_ref, xn_ref, alpha_ref, *, first):
    n = r_ref.shape[1]
    r = r_ref[...]
    hess = hess_ref[...]
    curved = za_ref[:, n:n + 1] + zb_ref[:, n:n + 1] + sc_ref[:, 1:2]
    alpha = sc_ref[:, 0:1] / curved
    if first:
        p = r
        xn_ref[...] = alpha * p
    else:
        p = r + sc_ref[:, 2:3] * p_ref[...]
        xn_ref[...] = x_ref[...] + alpha * p
    pn_ref[...] = p
    image = za_ref[:, :n] + zb_ref[:, :n] + hess * p
    r = r - alpha * image
    rn_ref[...] = r
    alpha_ref[...] = jnp.broadcast_to(alpha, alpha_ref.shape)
    store_flows(r, hess, p, (a0, a1, a2, a3), payload_ref)


def contingency(flows, k, w_ref, f_ref, out_ref):
    lane = lane_index((1, LANE))
    chosen = lane == out_ref[k]
    factors = jnp.where(chosen, -1.0, f_ref[k:k + 1, :])
    hit = jnp.sum(jnp.where(chosen, flows, 0.0), axis=1, keepdims=True)
    post = flows + factors * hit
    weighted = w_ref[k:k + 1, :] * post
    return chosen, factors, post, weighted


def lines_body(*refs, first, last):
    fa_ref, fb_ref, fp_ref, fx_ref, sc_ref, alpha_ref, w_ref, f_ref = refs[:8]
    mats = () if last else refs[8:12]
    out_ref = refs[8 if last else 12]
    z_ref, fpn_ref, fxn_ref, scn_ref = refs[9 if last else 13:]
    conts = w_ref.shape[0]
    rows = fa_ref.shape[0] // (conts + 1)
    top = conts * rows
    sums = fa_ref[top:, :] + fb_ref[top:, :]
    rr, base = sums[:, 0:1], sums[:, 1:2]
    if not first:
        beta = rr / sc_ref[:, 0:1]
        base = base + beta * (2.0 * sums[:, 2:3] + beta * sc_ref[:, 1:2])
        alpha = alpha_ref[:, 0:1]
    lane = lane_index((rows, LANE))
    packed = jnp.where(lane == 0, rr, 0.0) + jnp.where(lane == 1, base, 0.0)
    if not first:
        packed = packed + jnp.where(lane == 2, beta, 0.0)
    scn_ref[...] = packed
    curv = jnp.zeros((rows, 1), F32)
    backs = []
    for k in range(conts):
        span = slice(k * rows, (k + 1) * rows)
        flows = fa_ref[span, :] + fb_ref[span, :]
        if not first:
            before = fp_ref[span, :]
            fxn_ref[span, :] = fx_ref[span, :] + alpha * before
            flows = flows + beta * before
        else:
            fxn_ref[span, :] = jnp.zeros((rows, LANE), F32)
        fpn_ref[span, :] = flows
        chosen, factors, post, weighted = contingency(flows, k, w_ref, f_ref, out_ref)
        curv = curv + jnp.sum(post * weighted, axis=1, keepdims=True)
        if not last:
            total = jnp.sum(factors * weighted, axis=1, keepdims=True)
            backs.append(weighted + jnp.where(chosen, total, 0.0))
    if last:
        z_ref[...] = jnp.broadcast_to(curv, z_ref.shape)
    else:
        halves = from_lines(jnp.concatenate(backs, axis=1), mats)
        n = halves[0].shape[1]
        z_ref[:, :n] = halves[0]
        z_ref[:, n:2 * n] = halves[1]
        z_ref[:, 2 * n:] = jnp.broadcast_to(curv, (rows, LANE))


def finish_body(ca_ref, cb_ref, r_ref, p_ref, x_ref, sc_ref, fp_ref, fx_ref, w_ref, f_ref, out_ref,
                own_ref, send_ref):
    n = r_ref.shape[1] // 2
    rows = r_ref.shape[0]
    alpha = sc_ref[:, 0:1] / (ca_ref[:, 0:1] + cb_ref[:, 0:1] + sc_ref[:, 1:2])
    p = r_ref[...] + sc_ref[:, 2:3] * p_ref[...]
    x = x_ref[...] + alpha * p
    own_ref[:, :n] = x[:, :n]
    send_ref[:, :n] = x[:, n:]
    for k in range(w_ref.shape[0]):
        span = slice(k * rows, (k + 1) * rows)
        flows = fx_ref[span, :] + alpha * fp_ref[span, :]
        weighted = contingency(flows, k, w_ref, f_ref, out_ref)[3]
        own_ref[:, n + k * LANE:n + (k + 1) * LANE] = weighted
        send_ref[:, n + k * LANE:n + (k + 1) * LANE] = weighted


def place_body(own_ref, other_ref, side_ref, x_ref, w_ref):
    rows = own_ref.shape[0]
    n = x_ref.shape[1]
    side = side_ref[0]
    for which, ref in ((side, own_ref), (1 - side, other_ref)):
        at = pl.ds(pl.multiple_of(which * rows, 8), rows)
        x_ref[at, :] = ref[:, :n]
        for k in range(w_ref.shape[0]):
            w_ref[k, at, :] = ref[:, n + k * LANE:n + (k + 1) * LANE]


def per_device(right_sides, base_hessian, sensitivity, weights, outage_factors, outaged, *, scen, base):
    conts, n, lines = sensitivity.shape
    rhs = right_sides.shape[0]
    rows = rhs // 2
    outaged = outaged.astype(jnp.int32)

    def swap(value, axis, size, distance):
        return lax.ppermute(value, axis, [(i, i ^ distance) for i in range(size)])

    def butterfly(value, axis, size, distance):
        while 2 * distance < size:
            value = value + swap(value, axis, size, distance)
            distance *= 2
        return value, swap(value, axis, size, distance)

    side = lax.axis_index("scen") % 2
    other_a = swap(sensitivity, "scen", scen, 1)
    mine = lax.dynamic_slice_in_dim(right_sides, side * rows, rows, 0)
    theirs = lax.dynamic_slice_in_dim(right_sides, (1 - side) * rows, rows, 0)
    extra = jnp.concatenate([theirs, jnp.broadcast_to(base_hessian[None, :], (8, n))], axis=0)
    other = swap(extra, "scen", scen, 1)
    r = jnp.concatenate([mine, other[:rows]], axis=1)
    hess = jnp.concatenate([base_hessian[None, :], other[rows:rows + 1]], axis=1)
    mats = convert(sensitivity) + convert(other_a)

    flat = struct((conts * rows, LANE))
    state = struct((rows, 2 * n))
    scal = struct((rows, LANE))
    payload = struct(((conts + 1) * rows, LANE))
    wide = struct((rows, 2 * n + LANE))

    pay = call(first_body, payload, "first", r, hess, *mats)
    p = x = r
    fp = fx = jnp.zeros(flat.shape, F32)
    sc = alpha = jnp.zeros(scal.shape, F32)
    for it in range(ITERS):
        first, last = it == 0, it + 1 == ITERS
        fa, fb = butterfly(pay, "scen", scen, 2)
        tail = () if last else tuple(mats)
        z, fp, fx, sc = call(
            functools.partial(lines_body, first=first, last=last),
            [scal if last else wide, flat, flat, scal], "lines",
            fa, fb, fp, fx, sc, alpha, weights, outage_factors, *tail, outaged, scalars=1)
        za, zb = butterfly(z, "base", base, 1)
        if not last:
            pay, r, p, x, alpha = call(
                functools.partial(step_body, first=first),
                [payload, state, state, state, scal], "step",
                za, zb, r, p, x, sc, hess, *mats)
    both = struct((rows, n + conts * LANE))
    own, send = call(finish_body, [both, both], "finish", za, zb, r, p, x, sc, fp, fx,
                     weights, outage_factors, outaged, scalars=1)
    recv = swap(send, "scen", scen, 1)
    step, flow = call(place_body, [struct((rhs, n)), struct((conts, rhs, lines))], "place",
                      own, recv, side.astype(jnp.int32).reshape(1), scalars=1)
    return step, flow


def solution(mesh):
    placed = (
        P(None, "scen"),
        P("scen"),
        P("base", "scen", None),
        P("base", None),
        P("base", None),
        P("base"),
    )
    body = functools.partial(per_device, scen=mesh.shape["scen"], base=mesh.shape["base"])
    return jax.shard_map(
        body,
        mesh=mesh,
        in_specs=placed,
        out_specs=(P(None, "scen"), P("base", None, None)),
        check_vma=False,
    )
```

```python
import functools

import jax
import jax.numpy as jnp
from jax import lax
from jax.experimental import pallas as pl
from jax.experimental.pallas import tpu as pltpu
from jax.sharding import PartitionSpec as P

ITERS = 5
LANE = 128
F32 = jnp.float32
BF16 = jnp.bfloat16
VM = pl.BlockSpec(memory_space=pltpu.VMEM)
PARAMS = pltpu.CompilerParams(vmem_limit_bytes=24 * 1024 * 1024)


def call(body, out_shape, name, *args):
    many = isinstance(out_shape, (list, tuple))
    return pl.pallas_call(
        body,
        out_shape=out_shape,
        in_specs=[VM] * len(args),
        out_specs=[VM] * len(out_shape) if many else VM,
        compiler_params=PARAMS,
        name=name,
    )(*args)


def struct(shape, dtype=F32):
    return jax.ShapeDtypeStruct(shape, dtype)


def split(value):
    high = value.astype(BF16)
    low = (value - high.astype(F32)).astype(BF16)
    return high, low


def stacked(value):
    high, low = split(value)
    return jnp.concatenate([high, low], axis=0)


def lane_index(shape):
    return lax.broadcasted_iota(jnp.int32, shape, 1)


def convert_body(a_ref, high_ref, low_ref):
    for k in range(a_ref.shape[0]):
        high, low = split(a_ref[k])
        high_ref[:, k * LANE:(k + 1) * LANE] = high
        low_ref[:, k * LANE:(k + 1) * LANE] = low


def convert(a):
    k, n, m = a.shape
    shape = struct((n, k * m), BF16)
    return call(convert_body, [shape, shape], "convert", a)


def dot(lhs, rhs, rhs_dim):
    return lax.dot_general(lhs, rhs, (((1,), (rhs_dim,)), ((), ())), preferred_element_type=F32)


def to_lines(vector, mats):
    rows, n = vector.shape[0], vector.shape[1] // 2
    total = None
    for half in range(2):
        pair = stacked(vector[:, half * n:(half + 1) * n])
        for part in range(2):
            out = dot(pair, mats[2 * half + part][...], 0)
            total = out if total is None else total + out
    return total[:rows] + total[rows:]


def from_lines(lines, mats):
    rows = lines.shape[0]
    pair = stacked(lines)
    halves = []
    for half in range(2):
        out = dot(pair, mats[2 * half][...], 0) + dot(pair, mats[2 * half + 1][...], 0)
        halves.append(out[:rows] + out[rows:])
    return halves


def operator(w, f, out):
    row = lax.broadcasted_iota(jnp.int32, (LANE, LANE), 0)
    col = lax.broadcasted_iota(jnp.int32, (LANE, LANE), 1)
    lane = lane_index((1, LANE))
    kept = jnp.where(lane == out, 0.0, f)
    gain = w * kept
    corner = jnp.sum(gain * kept, axis=1, keepdims=True)
    edge = jnp.where(row == out, gain, 0.0)
    inner = jnp.where(row == col, jnp.where(col == out, corner, w), 0.0)
    return inner + edge + edge.T


def fold_body(high_ref, low_ref, w_ref, f_ref, out_ref, bh_ref, bl_ref):
    for k in range(w_ref.shape[0]):
        span = slice(k * LANE, (k + 1) * LANE)
        op = operator(w_ref[k:k + 1, :], f_ref[k:k + 1, :], out_ref[k:k + 1, :])
        pair = stacked(op)
        main = dot(pair, high_ref[:, span], 1)
        rest = dot(pair[:LANE], low_ref[:, span], 1)
        high, low = split(main[:LANE] + (main[LANE:] + rest))
        bh_ref[span, :] = high
        bl_ref[span, :] = low


def fold(pair, w, f, out):
    n, m = pair[0].shape
    shape = struct((m, n), BF16)
    return call(fold_body, [shape, shape], "fold", *pair, w, f, out)


def store_flows(vector, hess, previous, mats, payload_ref):
    rows = vector.shape[0]
    lines = to_lines(vector, mats)
    conts = lines.shape[1] // LANE
    for k in range(conts):
        payload_ref[k * rows:(k + 1) * rows, :] = lines[:, k * LANE:(k + 1) * LANE]
    scaled = hess * vector
    first = jnp.sum(vector * vector, axis=1, keepdims=True)
    second = jnp.sum(scaled * vector, axis=1, keepdims=True)
    lane = lane_index((rows, LANE))
    packed = jnp.where(lane == 0, first, 0.0) + jnp.where(lane == 1, second, 0.0)
    if previous is not None:
        third = jnp.sum(scaled * previous, axis=1, keepdims=True)
        packed = packed + jnp.where(lane == 2, third, 0.0)
    payload_ref[conts * rows:(conts + 1) * rows, :] = packed


def first_body(r_ref, hess_ref, a0, a1, a2, a3, payload_ref):
    store_flows(r_ref[...], hess_ref[...], None, (a0, a1, a2, a3), payload_ref)


def merged(za_ref, zb_ref, rows, chunks):
    def block(ref, at):
        return ref[at * rows:(at + 1) * rows, :]

    own = [block(za_ref, c) + block(zb_ref, chunks + c) for c in range(chunks)]
    other = [block(za_ref, chunks + c) + block(zb_ref, c) for c in range(chunks)]
    curved = block(za_ref, 2 * chunks) + block(zb_ref, 2 * chunks)
    return jnp.concatenate(own + other, axis=1), curved


def step_body(za_ref, zb_ref, r_ref, p_ref, x_ref, sc_ref, hess_ref, a0, a1, a2, a3,
              payload_ref, rn_ref, pn_ref, xn_ref, alpha_ref, *, first):
    rows, n = r_ref.shape
    r = r_ref[...]
    hess = hess_ref[...]
    image, curved = merged(za_ref, zb_ref, rows, n // 2 // LANE)
    alpha = sc_ref[:, 0:1] / (curved[:, 0:1] + sc_ref[:, 1:2])
    if first:
        p = r
        xn_ref[...] = alpha * p
    else:
        p = r + sc_ref[:, 2:3] * p_ref[...]
        xn_ref[...] = x_ref[...] + alpha * p
    pn_ref[...] = p
    r = r - alpha * (image + hess * p)
    rn_ref[...] = r
    alpha_ref[...] = jnp.broadcast_to(alpha, alpha_ref.shape)
    store_flows(r, hess, p, (a0, a1, a2, a3), payload_ref)


def weigh(flows, k, w_ref, f_ref, out_ref):
    chosen = lane_index((1, LANE)) == out_ref[k:k + 1, :]
    factors = jnp.where(chosen, -1.0, f_ref[k:k + 1, :])
    hit = jnp.sum(jnp.where(chosen, flows, 0.0), axis=1, keepdims=True)
    post = flows + factors * hit
    return post, w_ref[k:k + 1, :] * post


def lines_body(*refs, count, first, last):
    parts, refs = refs[:count], refs[count:]
    fp_ref, fx_ref, sc_ref, alpha_ref, w_ref, f_ref, out_ref = refs[:7]
    mats = () if last else refs[7:11]
    z_ref, fpn_ref, fxn_ref, scn_ref = refs[7 if last else 11:]
    conts = w_ref.shape[0]
    rows = parts[0].shape[0] // (conts + 1)

    def total(at):
        values = [ref[at:at + rows, :] for ref in parts]
        while len(values) > 1:
            values = [values[i] + values[i + 1] for i in range(0, len(values), 2)]
        return values[0]

    sums = total(conts * rows)
    rr, base = sums[:, 0:1], sums[:, 1:2]
    if not first:
        beta = rr / sc_ref[:, 0:1]
        base = base + beta * (2.0 * sums[:, 2:3] + beta * sc_ref[:, 1:2])
        alpha = alpha_ref[:, 0:1]
    lane = lane_index((rows, LANE))
    packed = jnp.where(lane == 0, rr, 0.0) + jnp.where(lane == 1, base, 0.0)
    if not first:
        packed = packed + jnp.where(lane == 2, beta, 0.0)
    scn_ref[...] = packed
    curv = jnp.zeros((rows, LANE), F32)
    flat = []
    for k in range(conts):
        span = slice(k * rows, (k + 1) * rows)
        flows = total(k * rows)
        if not first:
            before = fp_ref[span, :]
            fxn_ref[span, :] = fx_ref[span, :] + alpha * before
            flows = flows + beta * before
        else:
            fxn_ref[span, :] = jnp.zeros((rows, LANE), F32)
        fpn_ref[span, :] = flows
        post, weighted = weigh(flows, k, w_ref, f_ref, out_ref)
        curv = curv + post * weighted
        flat.append(flows)
    curv = jnp.broadcast_to(jnp.sum(curv, axis=1, keepdims=True), (rows, LANE))
    if last:
        z_ref[...] = curv
    else:
        halves = from_lines(jnp.concatenate(flat, axis=1), mats)
        chunks = halves[0].shape[1] // LANE
        for half in range(2):
            for c in range(chunks):
                at = (half * chunks + c) * rows
                z_ref[at:at + rows, :] = halves[half][:, c * LANE:(c + 1) * LANE]
        z_ref[2 * chunks * rows:, :] = curv


def finish_body(ca_ref, cb_ref, r_ref, p_ref, x_ref, sc_ref, fp_ref, fx_ref, w_ref, f_ref, out_ref,
                own_ref, send_ref):
    n = r_ref.shape[1] // 2
    rows = r_ref.shape[0]
    alpha = sc_ref[:, 0:1] / (ca_ref[:, 0:1] + cb_ref[:, 0:1] + sc_ref[:, 1:2])
    p = r_ref[...] + sc_ref[:, 2:3] * p_ref[...]
    x = x_ref[...] + alpha * p
    own_ref[:, :n] = x[:, :n]
    send_ref[:, :n] = x[:, n:]
    for k in range(w_ref.shape[0]):
        span = slice(k * rows, (k + 1) * rows)
        flows = fx_ref[span, :] + alpha * fp_ref[span, :]
        weighted = weigh(flows, k, w_ref, f_ref, out_ref)[1]
        own_ref[:, n + k * LANE:n + (k + 1) * LANE] = weighted
        send_ref[:, n + k * LANE:n + (k + 1) * LANE] = weighted


def place_body(own_ref, other_ref, part_ref, x_ref, w_ref):
    rows = own_ref.shape[0]
    n = x_ref.shape[1]
    upper = part_ref[0:1, 0:1] > 0
    for low in range(2):
        one, two = (other_ref, own_ref) if low == 0 else (own_ref, other_ref)
        value = jnp.where(upper, one[...], two[...])
        at = slice(low * rows, (low + 1) * rows)
        x_ref[at, :] = value[:, :n]
        for k in range(w_ref.shape[0]):
            w_ref[k, at, :] = value[:, n + k * LANE:n + (k + 1) * LANE]


def per_device(right_sides, base_hessian, sensitivity, weights, outage_factors, outaged, *, scen, base):
    conts, n, lines = sensitivity.shape
    rhs = right_sides.shape[0]
    rows = rhs // 2
    half = n // LANE * rows
    spread = jnp.broadcast_to(outaged.astype(jnp.int32)[:, None], (conts, lines))

    def half_of(s, b):
        return (s.bit_count() + b.bit_count()) & 1

    def swap(value, *steps):
        pairs = []
        for s in range(scen):
            for b in range(base):
                along, across = steps[half_of(s, b) % len(steps)]
                pairs.append((s * base + b, (s ^ along) * base + (b ^ across)))
        return lax.ppermute(value, ("scen", "base"), pairs)

    def over_scen(value):
        bit = 2
        while 4 * bit < scen:
            value = value + swap(value, (bit | 1, 0))
            bit *= 2
        if 2 * bit < scen:
            one, two = (bit | 1, 0), (2 * bit | 1, 0)
            return [value, swap(value, one, two), swap(value, two, one), swap(value, (3 * bit, 0))]
        return [value, swap(value, (bit | 1, 0))]

    def over_base(value):
        bits = [1 << i for i in range((base - 1).bit_length())]
        for i, bit in enumerate(bits):
            got = swap(value, (1, bit), (1, bits[(i + 1) % len(bits)]))
            if i + 1 == len(bits):
                return value, got
            if got.shape[0] > 2 * half:
                got = jnp.concatenate([got[half:2 * half], got[:half], got[2 * half:]], axis=0)
            value = value + got

    place = lax.axis_index("scen") * base + lax.axis_index("base")
    bits = (scen * base - 1).bit_length()
    part = sum((place >> i) & 1 for i in range(bits)) & 1
    other_a = swap(sensitivity, (1, 0))
    mine = lax.dynamic_slice_in_dim(right_sides, part * rows, rows, 0)
    theirs = lax.dynamic_slice_in_dim(right_sides, (1 - part) * rows, rows, 0)
    extra = jnp.concatenate([theirs, jnp.broadcast_to(base_hessian[None, :], (8, n))], axis=0)
    other = swap(extra, (1, 0))
    r = jnp.concatenate([mine, other[:rows]], axis=1)
    hess = jnp.concatenate([base_hessian[None, :], other[rows:rows + 1]], axis=1)
    pairs = convert(sensitivity), convert(other_a)
    mats = [*pairs[0], *pairs[1]]

    flat = struct((conts * rows, LANE))
    state = struct((rows, 2 * n))
    scal = struct((rows, LANE))
    payload = struct(((conts + 1) * rows, LANE))
    wide = struct((2 * half + rows, LANE))

    pay = call(first_body, payload, "first", r, hess, *mats)
    table = (weights, outage_factors, spread)
    folded = [*fold(pairs[0], *table), *fold(pairs[1], *table)]
    p = x = r
    fp = fx = jnp.zeros(flat.shape, F32)
    sc = alpha = jnp.zeros(scal.shape, F32)
    for it in range(ITERS):
        first, last = it == 0, it + 1 == ITERS
        sent = over_scen(pay)
        tail = () if last else tuple(folded)
        z, fp, fx, sc = call(
            functools.partial(lines_body, count=len(sent), first=first, last=last),
            [scal if last else wide, flat, flat, scal], "lines",
            *sent, fp, fx, sc, alpha, *table, *tail)
        za, zb = over_base(z)
        if not last:
            pay, r, p, x, alpha = call(
                functools.partial(step_body, first=first),
                [payload, state, state, state, scal], "step",
                za, zb, r, p, x, sc, hess, *mats)
    both = struct((rows, n + conts * LANE))
    own, send = call(finish_body, [both, both], "finish", za, zb, r, p, x, sc, fp, fx, *table)
    recv = swap(send, (1, 0))
    which = jnp.broadcast_to(part.astype(jnp.int32), (8, LANE))
    step, flow = call(place_body, [struct((rhs, n)), struct((conts, rhs, lines))], "place", own, recv, which)
    return step, flow


def solution(mesh):
    placed = (
        P(None, "scen"),
        P("scen"),
        P("base", "scen", None),
        P("base", None),
        P("base", None),
        P("base"),
    )
    body = functools.partial(per_device, scen=mesh.shape["scen"], base=mesh.shape["base"])
    return jax.shard_map(
        body,
        mesh=mesh,
        in_specs=placed,
        out_specs=(P(None, "scen"), P("base", None, None)),
        check_vma=False,
    )
```

```python
import functools

import jax
import jax.numpy as jnp
from jax import lax
from jax.experimental import pallas as pl
from jax.experimental.pallas import tpu as pltpu
from jax.sharding import PartitionSpec as P

ITERS = 5
LANE = 128
F32 = jnp.float32
BF16 = jnp.bfloat16
VM = pl.BlockSpec(memory_space=pltpu.VMEM)
PARAMS = pltpu.CompilerParams(vmem_limit_bytes=24 * 1024 * 1024)


def call(body, out_shape, name, *args):
    many = isinstance(out_shape, (list, tuple))
    return pl.pallas_call(
        body,
        out_shape=out_shape,
        in_specs=[VM] * len(args),
        out_specs=[VM] * len(out_shape) if many else VM,
        compiler_params=PARAMS,
        name=name,
    )(*args)


def struct(shape, dtype=F32):
    return jax.ShapeDtypeStruct(shape, dtype)


def split(value):
    high = value.astype(BF16)
    low = (value - high.astype(F32)).astype(BF16)
    return high, low


def stacked(value):
    high, low = split(value)
    return jnp.concatenate([high, low], axis=0)


def lane_index(shape):
    return lax.broadcasted_iota(jnp.int32, shape, 1)


def pack(columns):
    lane = lane_index((8, LANE))
    block = jnp.zeros((8, LANE), F32)
    at = 0
    for column in columns:
        for row in range(0, column.shape[0], 8):
            block = jnp.where(lane == at, column[row:row + 8], block)
            at += 1
    return block


def unpack(block, rows, index):
    groups = rows // 8
    return jnp.concatenate([block[:, index * groups + g:index * groups + g + 1] for g in range(groups)], axis=0)


def convert_body(a_ref, high_ref, low_ref):
    for k in range(a_ref.shape[0]):
        high, low = split(a_ref[k])
        high_ref[:, k * LANE:(k + 1) * LANE] = high
        low_ref[:, k * LANE:(k + 1) * LANE] = low


def convert(a):
    k, n, m = a.shape
    shape = struct((n, k * m), BF16)
    return call(convert_body, [shape, shape], "convert", a)


def dot(lhs, rhs, rhs_dim):
    return lax.dot_general(lhs, rhs, (((1,), (rhs_dim,)), ((), ())), preferred_element_type=F32)


def to_lines(vector, mats):
    count = len(mats) // 2
    rows, n = vector.shape[0], vector.shape[1] // count
    total = None
    for half in range(count):
        pair = stacked(vector[:, half * n:(half + 1) * n])
        for part in range(2):
            out = dot(pair, mats[2 * half + part][...], 0)
            total = out if total is None else total + out
    return total[:rows] + total[rows:]


def from_lines(lines, mats):
    rows = lines.shape[0]
    pair = stacked(lines)
    halves = []
    for half in range(2):
        out = dot(pair, mats[2 * half][...], 0) + dot(pair, mats[2 * half + 1][...], 0)
        halves.append(out[:rows] + out[rows:])
    return halves


def operator(w, f, out):
    row = lax.broadcasted_iota(jnp.int32, (LANE, LANE), 0)
    col = lax.broadcasted_iota(jnp.int32, (LANE, LANE), 1)
    lane = lane_index((1, LANE))
    kept = jnp.where(lane == out, 0.0, f)
    gain = w * kept
    corner = jnp.sum(gain * kept, axis=1, keepdims=True)
    edge = jnp.where(row == out, gain, 0.0)
    inner = jnp.where(row == col, jnp.where(col == out, corner, w), 0.0)
    return inner + edge + edge.T


def fold_body(high_ref, low_ref, w_ref, f_ref, out_ref, bh_ref, bl_ref):
    for k in range(w_ref.shape[0]):
        span = slice(k * LANE, (k + 1) * LANE)
        op = operator(w_ref[k:k + 1, :], f_ref[k:k + 1, :], out_ref[k:k + 1, :])
        pair = stacked(op)
        main = dot(pair, high_ref[:, span], 1)
        rest = dot(pair[:LANE], low_ref[:, span], 1)
        high, low = split(main[:LANE] + (main[LANE:] + rest))
        bh_ref[span, :] = high
        bl_ref[span, :] = low


def fold(pair, w, f, out):
    n, m = pair[0].shape
    shape = struct((m, n), BF16)
    return call(fold_body, [shape, shape], "fold", *pair, w, f, out)


def store(lines, columns, payload_ref):
    rows = lines.shape[0]
    conts = lines.shape[1] // LANE
    for k in range(conts):
        payload_ref[k * rows:(k + 1) * rows, :] = lines[:, k * LANE:(k + 1) * LANE]
    payload_ref[conts * rows:, :] = pack(columns)


def row_sum(value):
    return jnp.sum(value, axis=1, keepdims=True)


def half_of(s, b, bits=None):
    if bits is None:
        return (s.bit_count() + b.bit_count()) & 1
    return sum((s >> i) + (b >> i) for i in range(bits)) & 1


def prepare_body(a_hbm, b_hbm, hess_hbm, high_ref, low_ref, mine_ref, theirs_ref, own_ref, extra_ref,
                 held_ref, b_ref, hess_ref, sems, *, bits):
    conts = a_hbm.shape[0]
    copies = [pltpu.make_async_copy(a_hbm.at[k], held_ref.at[k], sems.at[k]) for k in range(conts)]
    first = pltpu.make_async_copy(b_hbm, b_ref, sems.at[conts])
    second = pltpu.make_async_copy(hess_hbm, hess_ref, sems.at[conts + 1])
    for copy in [first, second] + copies:
        copy.start()
    first.wait()
    second.wait()
    rows = b_ref.shape[0] // 2
    upper = half_of(lax.axis_index("scen"), lax.axis_index("base"), bits) == 1
    low, high = b_ref[:rows, :], b_ref[rows:, :]
    own_ref[...] = jnp.where(upper, high, low)
    extra_ref[:rows, :] = jnp.where(upper, low, high)
    hess = hess_ref[...]
    extra_ref[rows:, :] = jnp.broadcast_to(hess, (8, hess.shape[1]))
    for k in range(conts):
        copies[k].wait()
        one, two = split(held_ref[k])
        high_ref[:, k * LANE:(k + 1) * LANE] = one
        low_ref[:, k * LANE:(k + 1) * LANE] = two
    value = b_ref[...]
    lines = to_lines(value, (high_ref, low_ref))
    sums = row_sum(value * value), row_sum(hess * value * value)

    def chosen(value, flip):
        one, two = (value[:rows], value[rows:]) if flip else (value[rows:], value[:rows])
        return jnp.where(upper, one, two)

    for flip, ref in ((False, mine_ref), (True, theirs_ref)):
        store(chosen(lines, flip), [chosen(value, flip) for value in sums], ref)


def merged(refs, rows, chunks):
    lower = (lax.axis_index("scen") & 1) == 0
    sums = []
    for one, two in (refs[0:2], refs[2:4]):
        sums.append([one[c * rows:(c + 1) * rows, :] + two[c * rows:(c + 1) * rows, :] for c in range(chunks)])
    own = [jnp.where(lower, one, two) for one, two in zip(*sums)]
    other = [jnp.where(lower, two, one) for one, two in zip(*sums)]
    top = chunks * rows
    return jnp.concatenate(own + other, axis=1), unpack(refs[0][top:, :] + refs[1][top:, :], rows, 0)


def step_body(za_ref, zb_ref, zc_ref, zd_ref, r_ref, p_ref, x_ref, sc_ref, hess_ref, a0, a1, a2, a3,
              payload_ref, rn_ref, pn_ref, xn_ref, alpha_ref, *, first):
    rows, n = r_ref.shape
    r = r_ref[...]
    hess = hess_ref[...]
    image, curved = merged((za_ref, zb_ref, zc_ref, zd_ref), rows, n // 2 // LANE)
    alpha = sc_ref[:, 0:1] / (curved + sc_ref[:, 1:2])
    if first:
        p = r
        xn_ref[...] = alpha * p
    else:
        p = r + sc_ref[:, 2:3] * p_ref[...]
        xn_ref[...] = x_ref[...] + alpha * p
    pn_ref[...] = p
    r = r - alpha * (image + hess * p)
    rn_ref[...] = r
    alpha_ref[...] = jnp.broadcast_to(alpha, alpha_ref.shape)
    scaled = hess * r
    store(to_lines(r, (a0, a1, a2, a3)), [row_sum(r * r), row_sum(scaled * r), row_sum(scaled * p)], payload_ref)


def weigh(flows, k, w_ref, f_ref, out_ref):
    chosen = lane_index((1, LANE)) == out_ref[k:k + 1, :]
    factors = jnp.where(chosen, -1.0, f_ref[k:k + 1, :])
    hit = jnp.sum(jnp.where(chosen, flows, 0.0), axis=1, keepdims=True)
    post = flows + factors * hit
    return post, w_ref[k:k + 1, :] * post


def lines_body(*refs, count, first, last):
    parts, refs = refs[:count], refs[count:]
    fp_ref, fx_ref, sc_ref, alpha_ref, w_ref, f_ref, out_ref = refs[:7]
    mats = () if last else refs[7:11]
    *z_refs, fpn_ref, fxn_ref, scn_ref = refs[7 if last else 11:]
    conts = w_ref.shape[0]
    rows = parts[0].shape[0] // conts // 8 * 8

    def total(at, size):
        values = [ref[at:at + size, :] for ref in parts]
        while len(values) > 1:
            values = [values[i] + values[i + 1] for i in range(0, len(values), 2)]
        return values[0]

    sums = total(conts * rows, 8)
    rr, base = unpack(sums, rows, 0), unpack(sums, rows, 1)
    if not first:
        beta = rr / sc_ref[:, 0:1]
        base = base + beta * (2.0 * unpack(sums, rows, 2) + beta * sc_ref[:, 1:2])
        alpha = alpha_ref[:, 0:1]
    lane = lane_index((rows, LANE))
    packed = jnp.where(lane == 0, rr, 0.0) + jnp.where(lane == 1, base, 0.0)
    if not first:
        packed = packed + jnp.where(lane == 2, beta, 0.0)
    scn_ref[...] = packed
    curv = jnp.zeros((rows, LANE), F32)
    flat = []
    for k in range(conts):
        span = slice(k * rows, (k + 1) * rows)
        flows = total(k * rows, rows)
        if not first:
            before = fp_ref[span, :]
            fxn_ref[span, :] = fx_ref[span, :] + alpha * before
            flows = flows + beta * before
        else:
            fxn_ref[span, :] = jnp.zeros((rows, LANE), F32)
        fpn_ref[span, :] = flows
        post, weighted = weigh(flows, k, w_ref, f_ref, out_ref)
        curv = curv + post * weighted
        flat.append(flows)
    curv = pack([row_sum(curv)])
    if last:
        z_refs[0][...] = curv
    else:
        halves = from_lines(jnp.concatenate(flat, axis=1), mats)
        lower = (lax.axis_index("scen") & 1) == 0
        own, other = halves
        chunks = own.shape[1] // LANE
        for z_ref, value in zip(z_refs, (jnp.where(lower, own, other), jnp.where(lower, other, own))):
            for c in range(chunks):
                z_ref[c * rows:(c + 1) * rows, :] = value[:, c * LANE:(c + 1) * LANE]
        z_refs[0][chunks * rows:, :] = curv


def finish_body(ca_ref, cb_ref, r_ref, p_ref, x_ref, sc_ref, fp_ref, fx_ref, w_ref, f_ref, out_ref,
                own_ref, send_ref):
    n = r_ref.shape[1] // 2
    rows = r_ref.shape[0]
    alpha = sc_ref[:, 0:1] / (unpack(ca_ref[...] + cb_ref[...], rows, 0) + sc_ref[:, 1:2])
    p = r_ref[...] + sc_ref[:, 2:3] * p_ref[...]
    x = x_ref[...] + alpha * p
    own_ref[:, :n] = x[:, :n]
    send_ref[:, :n] = x[:, n:]
    for k in range(w_ref.shape[0]):
        span = slice(k * rows, (k + 1) * rows)
        flows = fx_ref[span, :] + alpha * fp_ref[span, :]
        weighted = weigh(flows, k, w_ref, f_ref, out_ref)[1]
        own_ref[:, n + k * LANE:n + (k + 1) * LANE] = weighted
        send_ref[:, n + k * LANE:n + (k + 1) * LANE] = weighted


def place_body(own_ref, other_ref, part_ref, x_ref, w_ref):
    rows = own_ref.shape[0]
    n = x_ref.shape[1]
    upper = part_ref[0:1, 0:1] > 0
    for low in range(2):
        one, two = (other_ref, own_ref) if low == 0 else (own_ref, other_ref)
        value = jnp.where(upper, one[...], two[...])
        at = slice(low * rows, (low + 1) * rows)
        x_ref[at, :] = value[:, :n]
        for k in range(w_ref.shape[0]):
            w_ref[k, at, :] = value[:, n + k * LANE:n + (k + 1) * LANE]


def per_device(right_sides, base_hessian, sensitivity, weights, outage_factors, outaged, *, scen, base):
    conts, n, lines = sensitivity.shape
    rhs = right_sides.shape[0]
    rows = rhs // 2
    half = n // LANE * rows
    spread = jnp.broadcast_to(outaged.astype(jnp.int32)[:, None], (conts, lines))

    def swap(value, *steps):
        pairs = []
        for s in range(scen):
            for b in range(base):
                along, across = steps[half_of(s, b) % len(steps)]
                pairs.append((s * base + b, (s ^ along) * base + (b ^ across)))
        return lax.ppermute(value, ("scen", "base"), pairs)

    def over_scen(value):
        bit = 2
        while 4 * bit < scen:
            value = value + swap(value, (bit | 1, 0))
            bit *= 2
        if 2 * bit < scen:
            one, two = (bit | 1, 0), (2 * bit | 1, 0)
            return [value, swap(value, one, two), swap(value, two, one), swap(value, (3 * bit, 0))]
        return [value, swap(value, (bit | 1, 0))]

    def over_base(values):
        order = [1 << i for i in range((base - 1).bit_length())]
        for i in range(len(order)):
            got = []
            for value in values:
                steps = [(1, order[(i + turn) % len(order)]) for turn in (0, 1)]
                got.append(swap(value, *steps))
            if i + 1 == len(order):
                return [v for both in zip(values, got) for v in both]
            values = [value + new for value, new in zip(values, got)]

    bits = max(scen, base).bit_length()
    part = half_of(lax.axis_index("scen"), lax.axis_index("base"), bits)
    flat = struct((conts * rows, LANE))
    state = struct((rows, 2 * n))
    scal = struct((rows, LANE))
    payload = struct((conts * rows + 8, LANE))
    wide = [struct((half + 8, LANE)), struct((half, LANE))]
    block = struct((8, LANE))

    other_a = swap(sensitivity, (1, 0))
    matrix = struct((n, conts * lines), BF16)
    high, low, mine, theirs, own, extra = pl.pallas_call(
        functools.partial(prepare_body, bits=bits),
        out_shape=[matrix, matrix, payload, payload, struct((rows, n)), struct((rows + 8, n))],
        in_specs=[pl.BlockSpec(memory_space=pltpu.HBM)] * 3,
        out_specs=[VM] * 6,
        scratch_shapes=[
            pltpu.VMEM(sensitivity.shape, F32),
            pltpu.VMEM(right_sides.shape, F32),
            pltpu.VMEM((1, n), F32),
            pltpu.SemaphoreType.DMA((conts + 2,)),
        ],
        compiler_params=PARAMS,
        name="prepare",
    )(*[pltpu.with_memory_space_constraint(v, pltpu.HBM) for v in (sensitivity, right_sides, base_hessian.reshape(1, n))])
    pay = mine + swap(theirs, (1, 0))
    other = swap(extra, (1, 0))
    r = jnp.concatenate([own, other[:rows]], axis=1)
    hess = jnp.concatenate([base_hessian[None, :], other[rows:rows + 1]], axis=1)
    pairs = (high, low), convert(other_a)
    mats = [*pairs[0], *pairs[1]]

    table = (weights, outage_factors, spread)
    folded = [*fold(pairs[0], *table), *fold(pairs[1], *table)]
    p = x = r
    fp = fx = jnp.zeros(flat.shape, F32)
    sc = alpha = jnp.zeros(scal.shape, F32)
    for it in range(ITERS):
        first, last = it == 0, it + 1 == ITERS
        sent = over_scen(pay)
        tail = () if last else tuple(folded)
        *z, fp, fx, sc = call(
            functools.partial(lines_body, count=len(sent), first=first, last=last),
            [*([block] if last else wide), flat, flat, scal], "lines",
            *sent, fp, fx, sc, alpha, *table, *tail)
        z = over_base(z)
        if not last:
            pay, r, p, x, alpha = call(
                functools.partial(step_body, first=first),
                [payload, state, state, state, scal], "step",
                *z, r, p, x, sc, hess, *mats)
    both = struct((rows, n + conts * LANE))
    own, send = call(finish_body, [both, both], "finish", *z, r, p, x, sc, fp, fx, *table)
    recv = swap(send, (1, 0))
    which = jnp.broadcast_to(part.astype(jnp.int32), (8, LANE))
    step, flow = call(place_body, [struct((rhs, n)), struct((conts, rhs, lines))], "place", own, recv, which)
    return step, flow


def solution(mesh):
    placed = (
        P(None, "scen"),
        P("scen"),
        P("base", "scen", None),
        P("base", None),
        P("base", None),
        P("base"),
    )
    body = functools.partial(per_device, scen=mesh.shape["scen"], base=mesh.shape["base"])
    return jax.shard_map(
        body,
        mesh=mesh,
        in_specs=placed,
        out_specs=(P(None, "scen"), P("base", None, None)),
        check_vma=False,
    )
```

```python
import functools

import jax
import jax.numpy as jnp
from jax import lax
from jax.experimental import pallas as pl
from jax.experimental.pallas import tpu as pltpu
from jax.sharding import PartitionSpec as P

ITERS = 5
LANE = 128
F32 = jnp.float32
BF16 = jnp.bfloat16
VM = pl.BlockSpec(memory_space=pltpu.VMEM)
PARAMS = pltpu.CompilerParams(vmem_limit_bytes=24 * 1024 * 1024)


def call(body, out_shape, name, *args):
    many = isinstance(out_shape, (list, tuple))
    return pl.pallas_call(
        body,
        out_shape=out_shape,
        in_specs=[VM] * len(args),
        out_specs=[VM] * len(out_shape) if many else VM,
        compiler_params=PARAMS,
        name=name,
    )(*args)


def struct(shape, dtype=F32):
    return jax.ShapeDtypeStruct(shape, dtype)


def split(value):
    high = value.astype(BF16)
    low = (value - high.astype(F32)).astype(BF16)
    return high, low


def stacked(value):
    high, low = split(value)
    return jnp.concatenate([high, low], axis=0)


def lane_index(shape):
    return lax.broadcasted_iota(jnp.int32, shape, 1)


def pack(columns):
    lane = lane_index((8, LANE))
    block = jnp.zeros((8, LANE), F32)
    at = 0
    for column in columns:
        for row in range(0, column.shape[0], 8):
            block = jnp.where(lane == at, column[row:row + 8], block)
            at += 1
    return block


def unpack(block, rows, index):
    groups = rows // 8
    return jnp.concatenate([block[:, index * groups + g:index * groups + g + 1] for g in range(groups)], axis=0)


def core():
    return lax.axis_index("scen") & 1


def with_slot(slot, refs, body):
    own = core() == slot

    @pl.when(own)
    def _():
        body(*refs[:2])

    @pl.when(jnp.logical_not(own))
    def _():
        body(*refs[2:])


def dot(lhs, rhs, rhs_dim):
    return lax.dot_general(lhs, rhs, (((1,), (rhs_dim,)), ((), ())), preferred_element_type=F32)


def to_lines(vector, high_ref, low_ref):
    rows = vector.shape[0]
    pair = stacked(vector)
    total = dot(pair, high_ref[...], 0) + dot(pair, low_ref[...], 0)
    return total[:rows] + total[rows:]


def from_lines(pair, z_ref, high_ref, low_ref):
    rows = pair.shape[0] // 2
    total = dot(pair, high_ref[...], 0) + dot(pair, low_ref[...], 0)
    image = total[:rows] + total[rows:]
    for c in range(image.shape[1] // LANE):
        z_ref[c * rows:(c + 1) * rows, :] = image[:, c * LANE:(c + 1) * LANE]


def operator(w, f, out):
    row = lax.broadcasted_iota(jnp.int32, (LANE, LANE), 0)
    col = lax.broadcasted_iota(jnp.int32, (LANE, LANE), 1)
    lane = lane_index((1, LANE))
    kept = jnp.where(lane == out, 0.0, f)
    gain = w * kept
    corner = jnp.sum(gain * kept, axis=1, keepdims=True)
    edge = jnp.where(row == out, gain, 0.0)
    inner = jnp.where(row == col, jnp.where(col == out, corner, w), 0.0)
    return inner + edge + edge.T


def fold_one(k, high_ref, low_ref, w_ref, f_ref, out_ref, bh_ref, bl_ref):
    span = slice(k * LANE, (k + 1) * LANE)
    op = operator(w_ref[k:k + 1, :], f_ref[k:k + 1, :], out_ref[k:k + 1, :])
    pair = stacked(op)
    main = dot(pair, high_ref[:, span], 1)
    rest = dot(pair[:LANE], low_ref[:, span], 1)
    high, low = split(main[:LANE] + (main[LANE:] + rest))
    bh_ref[span, :] = high
    bl_ref[span, :] = low


def fold_body(high_ref, low_ref, w_ref, f_ref, out_ref, bh_ref, bl_ref):
    for k in range(w_ref.shape[0]):
        fold_one(k, high_ref, low_ref, w_ref, f_ref, out_ref, bh_ref, bl_ref)


def reads(a_hbm, held_ref, sems):
    return [pltpu.make_async_copy(a_hbm.at[k], held_ref.at[k], sems.at[k]) for k in range(a_hbm.shape[0])]


def convert_one(k, held_ref, high_ref, low_ref):
    high, low = split(held_ref[k])
    high_ref[:, k * LANE:(k + 1) * LANE] = high
    low_ref[:, k * LANE:(k + 1) * LANE] = low


def absorb_body(a_hbm, w_ref, f_ref, out_ref, high_ref, low_ref, bh_ref, bl_ref, held_ref, sems):
    copies = reads(a_hbm, held_ref, sems)
    for copy in copies:
        copy.start()
    for k, copy in enumerate(copies):
        copy.wait()
        convert_one(k, held_ref, high_ref, low_ref)
        fold_one(k, high_ref, low_ref, w_ref, f_ref, out_ref, bh_ref, bl_ref)


def fold(pair, w, f, out):
    n, m = pair[0].shape
    shape = struct((m, n), BF16)
    return call(fold_body, [shape, shape], "fold", *pair, w, f, out)


def store(lines, columns, payload_ref):
    rows = lines.shape[0]
    conts = lines.shape[1] // LANE
    for k in range(conts):
        payload_ref[k * rows:(k + 1) * rows, :] = lines[:, k * LANE:(k + 1) * LANE]
    if columns is not None:
        payload_ref[conts * rows:, :] = pack(columns)


def row_sum(value):
    return jnp.sum(value, axis=1, keepdims=True)


def flips(step, scen):
    return (step & (scen // 2 - 1)).bit_count() & 1


def half_of(s, b, scen, bits):
    s = s & (scen // 2 - 1)
    return sum((s >> i) + (b >> i) for i in range(bits)) & 1


def prepare_body(a_hbm, b_hbm, hess_hbm, high_ref, low_ref, mine_ref, theirs_ref, own_ref, extra_ref,
                 held_ref, b_ref, hess_ref, sems, *, scen, bits):
    conts = a_hbm.shape[0]
    copies = reads(a_hbm, held_ref, sems)
    first = pltpu.make_async_copy(b_hbm, b_ref, sems.at[conts])
    second = pltpu.make_async_copy(hess_hbm, hess_ref, sems.at[conts + 1])
    for copy in [first, second] + copies:
        copy.start()
    first.wait()
    second.wait()
    rows = b_ref.shape[0] // 2
    upper = half_of(lax.axis_index("scen"), lax.axis_index("base"), scen, bits) == 1
    low, high = b_ref[:rows, :], b_ref[rows:, :]
    own_ref[...] = jnp.where(upper, high, low)
    extra_ref[:rows, :] = jnp.where(upper, low, high)
    hess = hess_ref[...]
    extra_ref[rows:, :] = jnp.broadcast_to(hess, (8, hess.shape[1]))
    for k in range(conts):
        copies[k].wait()
        convert_one(k, held_ref, high_ref, low_ref)
    value = b_ref[...]
    lines = to_lines(value, high_ref, low_ref)
    sums = row_sum(value * value), row_sum(hess * value * value)

    def chosen(value, flip):
        one, two = (value[:rows], value[rows:]) if flip else (value[rows:], value[:rows])
        return jnp.where(upper, one, two)

    for flip, ref in ((False, mine_ref), (True, theirs_ref)):
        store(chosen(lines, flip), [chosen(value, flip) for value in sums], ref)


def summed(za_ref, zb_ref, rows, n):
    blocks = [za_ref[c * rows:(c + 1) * rows, :] + zb_ref[c * rows:(c + 1) * rows, :] for c in range(n // LANE)]
    return jnp.concatenate(blocks, axis=1)


def step_body(*refs, slot, first):
    za_ref, zb_ref, r_ref, p_ref, x_ref, sc_ref, hess_ref = refs[:7]
    mats, refs = refs[7:11], refs[11:]
    rows, n = r_ref.shape
    r = r_ref[...]
    hess = hess_ref[...]
    if slot == 0:
        out_ref, sums_ref, rn_ref, pn_ref, xn_ref, alpha_ref = refs
        top = n // LANE * rows
        curved = unpack(za_ref[top:, :] + zb_ref[top:, :], rows, 0)
        alpha = sc_ref[:, 0:1] / (curved + sc_ref[:, 1:2])
        alpha_ref[...] = jnp.broadcast_to(alpha, alpha_ref.shape)
    else:
        alpha_in, share_ref, share_sums, out_ref, rn_ref, pn_ref, xn_ref = refs
        alpha = alpha_in[:, 0:1]
    if first:
        p = r
        xn_ref[...] = alpha * p
    else:
        p = r + sc_ref[:, 2:3] * p_ref[...]
        xn_ref[...] = x_ref[...] + alpha * p
    pn_ref[...] = p
    r = r - alpha * (summed(za_ref, zb_ref, rows, n) + hess * p)
    rn_ref[...] = r
    scaled = hess * r
    columns = [row_sum(r * r), row_sum(scaled * r), row_sum(scaled * p)]
    sums = pack(columns)
    if slot == 0:
        sums_ref[...] = sums

    def share(high_ref, low_ref):
        lines = to_lines(r, high_ref, low_ref)
        if slot == 0:
            out_ref[...] = lines
        else:
            store(lines + share_ref[...], None, out_ref)

    with_slot(slot, mats, share)
    if slot == 1:
        out_ref[out_ref.shape[0] - 8:, :] = sums + share_sums[...]


def weigh(flows, k, w_ref, f_ref, out_ref):
    chosen = lane_index((1, LANE)) == out_ref[k:k + 1, :]
    factors = jnp.where(chosen, -1.0, f_ref[k:k + 1, :])
    hit = jnp.sum(jnp.where(chosen, flows, 0.0), axis=1, keepdims=True)
    post = flows + factors * hit
    return post, w_ref[k:k + 1, :] * post


def lines_body(*refs, count, first, last):
    parts, refs = refs[:count], refs[count:]
    fp_ref, fx_ref, sc_ref, alpha_ref, w_ref, f_ref, out_ref = refs[:7]
    if last:
        z_ref, fpn_ref, fxn_ref, scn_ref = refs[7:]
    else:
        mats = refs[7:11]
        z_ref, pair_ref, fpn_ref, fxn_ref, scn_ref = refs[11:]
    conts = w_ref.shape[0]
    rows = parts[0].shape[0] // conts // 8 * 8

    def total(at, size):
        values = [ref[at:at + size, :] for ref in parts]
        if count == 4:
            values = [values[0], values[3], values[1], values[2]]
        while len(values) > 1:
            values = [values[i] + values[i + 1] for i in range(0, len(values), 2)]
        return values[0]

    sums = total(conts * rows, 8)
    rr, base = unpack(sums, rows, 0), unpack(sums, rows, 1)
    if not first:
        beta = rr / sc_ref[:, 0:1]
        base = base + beta * (2.0 * unpack(sums, rows, 2) + beta * sc_ref[:, 1:2])
        alpha = alpha_ref[:, 0:1]
    lane = lane_index((rows, LANE))
    packed = jnp.where(lane == 0, rr, 0.0) + jnp.where(lane == 1, base, 0.0)
    if not first:
        packed = packed + jnp.where(lane == 2, beta, 0.0)
    scn_ref[...] = packed
    curv = jnp.zeros((rows, LANE), F32)
    flat = []
    for k in range(conts):
        span = slice(k * rows, (k + 1) * rows)
        flows = total(k * rows, rows)
        if not first:
            before = fp_ref[span, :]
            fxn_ref[span, :] = fx_ref[span, :] + alpha * before
            flows = flows + beta * before
        else:
            fxn_ref[span, :] = jnp.zeros((rows, LANE), F32)
        fpn_ref[span, :] = flows
        post, weighted = weigh(flows, k, w_ref, f_ref, out_ref)
        curv = curv + post * weighted
        flat.append(flows)
    curv = pack([row_sum(curv)])
    if last:
        z_ref[...] = curv
    else:
        pair = stacked(jnp.concatenate(flat, axis=1))
        pair_ref[...] = pair
        z_ref[z_ref.shape[0] - 8:, :] = curv
        with_slot(0, mats, functools.partial(from_lines, pair, z_ref))


def image_body(pair_ref, b0, b1, b2, b3, z_ref):
    with_slot(1, (b0, b1, b2, b3), functools.partial(from_lines, pair_ref[...], z_ref))


def finish_body(ca_ref, cb_ref, r0, r1, p0, p1, x0, x1, sc_ref, fp_ref, fx_ref, w_ref, f_ref, out_ref,
                own_ref, send_ref):
    rows, n = r0.shape
    alpha = sc_ref[:, 0:1] / (unpack(ca_ref[...] + cb_ref[...], rows, 0) + sc_ref[:, 1:2])
    one, two = [x[...] + alpha * (r[...] + sc_ref[:, 2:3] * p[...]) for r, p, x in ((r0, p0, x0), (r1, p1, x1))]
    lower = core() == 0
    own_ref[:, :n] = jnp.where(lower, one, two)
    send_ref[:, :n] = jnp.where(lower, two, one)
    for k in range(w_ref.shape[0]):
        span = slice(k * rows, (k + 1) * rows)
        flows = fx_ref[span, :] + alpha * fp_ref[span, :]
        weighted = weigh(flows, k, w_ref, f_ref, out_ref)[1]
        own_ref[:, n + k * LANE:n + (k + 1) * LANE] = weighted
        send_ref[:, n + k * LANE:n + (k + 1) * LANE] = weighted


def place_body(own_ref, other_ref, part_ref, x_ref, w_ref):
    rows = own_ref.shape[0]
    n = x_ref.shape[1]
    upper = part_ref[0:1, 0:1] > 0
    for low in range(2):
        one, two = (other_ref, own_ref) if low == 0 else (own_ref, other_ref)
        value = jnp.where(upper, one[...], two[...])
        at = slice(low * rows, (low + 1) * rows)
        x_ref[at, :] = value[:, :n]
        for k in range(w_ref.shape[0]):
            w_ref[k, at, :] = value[:, n + k * LANE:n + (k + 1) * LANE]


def per_device(right_sides, base_hessian, sensitivity, weights, outage_factors, outaged, *, scen, base):
    conts, n, lines = sensitivity.shape
    rhs = right_sides.shape[0]
    rows = rhs // 2
    half = n // LANE * rows
    bits = max(scen, base).bit_length()
    spread = jnp.broadcast_to(outaged.astype(jnp.int32)[:, None], (conts, lines))

    def swap(value, *steps):
        pairs = []
        for s in range(scen):
            for b in range(base):
                along, across = steps[half_of(s, b, scen, bits) % len(steps)]
                pairs.append((s * base + b, (s ^ along) * base + (b ^ across)))
        return lax.ppermute(value, ("scen", "base"), pairs)

    def over_scen(value):
        bit = 2
        while 4 * bit < scen:
            value = value + swap(value, (bit | 1, 0))
            bit *= 2
        if 2 * bit < scen:
            one, two, both = (bit | 1, 0), (2 * bit, 0), (3 * bit | 1, 0)
            return [value, swap(value, both), swap(value, two), swap(value, one)]
        return [value, swap(value, (bit | 1, 0))]

    def over_base(values):
        order = [1 << i for i in range((base - 1).bit_length())]
        for i in range(len(order)):
            got = []
            for value in values:
                steps = [(1, order[(i + turn) % len(order)]) for turn in (0, 1)]
                got.append(swap(value, *steps))
            if i + 1 == len(order):
                return [v for both in zip(values, got) for v in both]
            values = [value + new for value, new in zip(values, got)]
            values[1:] = [lax.optimization_barrier((value, values[0]))[0] for value in values[1:]]

    part = half_of(lax.axis_index("scen"), lax.axis_index("base"), scen, bits)
    flat = struct((conts * rows, LANE))
    state = struct((rows, n))
    scal = struct((rows, LANE))
    payload = struct((conts * rows + 8, LANE))
    wide = [struct((half + 8, LANE)), struct((half, LANE))]
    share = struct((rows, conts * lines))
    pair = struct((2 * rows, conts * lines), BF16)
    block = struct((8, LANE))

    matrix = struct((n, conts * lines), BF16)
    high, low, mine, theirs, own, extra = pl.pallas_call(
        functools.partial(prepare_body, scen=scen, bits=bits),
        out_shape=[matrix, matrix, payload, payload, struct((rows, n)), struct((rows + 8, n))],
        in_specs=[pl.BlockSpec(memory_space=pltpu.HBM)] * 3,
        out_specs=[VM] * 6,
        scratch_shapes=[
            pltpu.VMEM(sensitivity.shape, F32),
            pltpu.VMEM(right_sides.shape, F32),
            pltpu.VMEM((1, n), F32),
            pltpu.SemaphoreType.DMA((conts + 2,)),
        ],
        compiler_params=PARAMS,
        name="prepare",
    )(*[pltpu.with_memory_space_constraint(v, pltpu.HBM) for v in (sensitivity, right_sides, base_hessian.reshape(1, n))])
    pay = mine + swap(theirs, (1, 0))
    held, late, pay = lax.optimization_barrier((sensitivity, extra, pay))
    other_a = swap(held, (1, 0))
    other = swap(late, (1, 0))
    lower = core() == 0

    def by_core(one, two):
        return [jnp.where(lower, one, two), jnp.where(lower, two, one)]

    r = by_core(own, other[:rows])
    hess = by_core(base_hessian[None, :], other[rows:rows + 1])
    table = (weights, outage_factors, spread)
    turned = struct((conts * lines, n), BF16)
    absorbed = pl.pallas_call(
        absorb_body,
        out_shape=[matrix, matrix, turned, turned],
        in_specs=[pl.BlockSpec(memory_space=pltpu.HBM)] + [VM] * 3,
        out_specs=[VM] * 4,
        scratch_shapes=[pltpu.VMEM(sensitivity.shape, F32), pltpu.SemaphoreType.DMA((conts,))],
        compiler_params=PARAMS,
        name="absorb",
    )(pltpu.with_memory_space_constraint(other_a, pltpu.HBM), *table)
    mats = [high, low, *absorbed[:2]]
    folded = [*fold(mats[:2], *table), *absorbed[2:]]
    p, x = list(r), list(r)
    fp = fx = jnp.zeros(flat.shape, F32)
    sc = alpha = jnp.zeros(scal.shape, F32)
    for it in range(ITERS):
        first, last = it == 0, it + 1 == ITERS
        sent = over_scen(pay)
        got = call(
            functools.partial(lines_body, count=len(sent), first=first, last=last),
            [*([block] if last else [wide[0], pair]), flat, flat, scal], "lines",
            *sent, fp, fx, sc, alpha, *table, *(() if last else folded))
        fp, fx, sc = got[-3:]
        if last:
            z = over_base(got[:1])
            break
        z = over_base([got[0], call(image_body, wide[1], "image", got[1], *folded)])
        share_lines, share_sums, r[0], p[0], x[0], alpha = call(
            functools.partial(step_body, slot=0, first=first),
            [share, block, state, state, state, scal], "step",
            *z[:2], r[0], p[0], x[0], sc, hess[0], *mats)
        pay, r[1], p[1], x[1] = call(
            functools.partial(step_body, slot=1, first=first),
            [payload, state, state, state], "step",
            *z[2:], r[1], p[1], x[1], sc, hess[1], *mats, alpha, share_lines, share_sums)
    both = struct((rows, n + conts * LANE))
    own, send = call(finish_body, [both, both], "finish", *z, *r, *p, *x, sc, fp, fx, *table)
    recv = swap(send, (1, 0))
    which = jnp.broadcast_to(part.astype(jnp.int32), (8, LANE))
    step, flow = call(place_body, [struct((rhs, n)), struct((conts, rhs, lines))], "place", own, recv, which)
    return step, flow


def solution(mesh):
    placed = (
        P(None, "scen"),
        P("scen"),
        P("base", "scen", None),
        P("base", None),
        P("base", None),
        P("base"),
    )
    body = functools.partial(per_device, scen=mesh.shape["scen"], base=mesh.shape["base"])
    return jax.shard_map(
        body,
        mesh=mesh,
        in_specs=placed,
        out_specs=(P(None, "scen"), P("base", None, None)),
        check_vma=False,
    )
```

```python
import functools

import jax
import jax.numpy as jnp
from jax import lax
from jax.experimental import pallas as pl
from jax.experimental.pallas import tpu as pltpu
from jax.sharding import PartitionSpec as P

ITERS = 5
LANE = 128
F32 = jnp.float32
BF16 = jnp.bfloat16
VM = pl.BlockSpec(memory_space=pltpu.VMEM)
PARAMS = pltpu.CompilerParams(vmem_limit_bytes=24 * 1024 * 1024)


def call(body, out_shape, name, *args):
    many = isinstance(out_shape, (list, tuple))
    return pl.pallas_call(
        body,
        out_shape=out_shape,
        in_specs=[VM] * len(args),
        out_specs=[VM] * len(out_shape) if many else VM,
        compiler_params=PARAMS,
        name=name,
    )(*args)


def struct(shape, dtype=F32):
    return jax.ShapeDtypeStruct(shape, dtype)


def split(value):
    high = value.astype(BF16)
    low = (value - high.astype(F32)).astype(BF16)
    return high, low


def stacked(value):
    high, low = split(value)
    return jnp.concatenate([high, low], axis=0)


def lane_index(shape):
    return lax.broadcasted_iota(jnp.int32, shape, 1)


def pack(columns):
    lane = lane_index((8, LANE))
    block = jnp.zeros((8, LANE), F32)
    at = 0
    for column in columns:
        for row in range(0, column.shape[0], 8):
            block = jnp.where(lane == at, column[row:row + 8], block)
            at += 1
    return block


def unpack(block, rows, index):
    groups = rows // 8
    return jnp.concatenate([block[:, index * groups + g:index * groups + g + 1] for g in range(groups)], axis=0)


def core():
    return lax.axis_index("scen") & 1


def with_slot(slot, refs, body):
    own = core() == slot

    @pl.when(own)
    def _():
        body(*refs[:2])

    @pl.when(jnp.logical_not(own))
    def _():
        body(*refs[2:])


def dot(lhs, rhs, rhs_dim):
    return lax.dot_general(lhs, rhs, (((1,), (rhs_dim,)), ((), ())), preferred_element_type=F32)


def to_lines(vector, high_ref, low_ref):
    rows = vector.shape[0]
    pair = stacked(vector)
    total = dot(pair, high_ref[...], 0) + dot(pair, low_ref[...], 0)
    return total[:rows] + total[rows:]


def from_lines(pair, z_ref, high_ref, low_ref):
    rows = pair.shape[0] // 2
    total = dot(pair, high_ref[...], 0) + dot(pair, low_ref[...], 0)
    image = total[:rows] + total[rows:]
    for c in range(image.shape[1] // LANE):
        z_ref[c * rows:(c + 1) * rows, :] = image[:, c * LANE:(c + 1) * LANE]


def operator(w, f, out):
    row = lax.broadcasted_iota(jnp.int32, (LANE, LANE), 0)
    col = lax.broadcasted_iota(jnp.int32, (LANE, LANE), 1)
    lane = lane_index((1, LANE))
    kept = jnp.where(lane == out, 0.0, f)
    gain = w * kept
    corner = jnp.sum(gain * kept, axis=1, keepdims=True)
    edge = jnp.where(row == out, gain, 0.0)
    inner = jnp.where(row == col, jnp.where(col == out, corner, w), 0.0)
    return inner + edge + edge.T


def fold_one(k, high_ref, low_ref, w_ref, f_ref, out_ref, bh_ref, bl_ref):
    span = slice(k * LANE, (k + 1) * LANE)
    op = operator(w_ref[k:k + 1, :], f_ref[k:k + 1, :], out_ref[k:k + 1, :])
    pair = stacked(op)
    main = dot(pair, high_ref[:, span], 1)
    rest = dot(pair[:LANE], low_ref[:, span], 1)
    high, low = split(main[:LANE] + (main[LANE:] + rest))
    bh_ref[span, :] = high
    bl_ref[span, :] = low


def fold_body(high_ref, low_ref, w_ref, f_ref, out_ref, bh_ref, bl_ref):
    for k in range(w_ref.shape[0]):
        fold_one(k, high_ref, low_ref, w_ref, f_ref, out_ref, bh_ref, bl_ref)


def reads(a_hbm, held_ref, sems):
    return [pltpu.make_async_copy(a_hbm.at[k], held_ref.at[k], sems.at[k]) for k in range(a_hbm.shape[0])]


def convert_one(k, held_ref, high_ref, low_ref):
    high, low = split(held_ref[k])
    high_ref[:, k * LANE:(k + 1) * LANE] = high
    low_ref[:, k * LANE:(k + 1) * LANE] = low


def absorb_body(a_hbm, own_high, own_low, w_ref, f_ref, out_ref, oh_ref, ol_ref,
                high_ref, low_ref, bh_ref, bl_ref, held_ref, sems):
    copies = reads(a_hbm, held_ref, sems)
    for copy in copies:
        copy.start()
    for k in range(len(copies)):
        fold_one(k, own_high, own_low, w_ref, f_ref, out_ref, oh_ref, ol_ref)
    for k, copy in enumerate(copies):
        copy.wait()
        convert_one(k, held_ref, high_ref, low_ref)
        fold_one(k, high_ref, low_ref, w_ref, f_ref, out_ref, bh_ref, bl_ref)


def fold(pair, w, f, out):
    n, m = pair[0].shape
    shape = struct((m, n), BF16)
    return call(fold_body, [shape, shape], "fold", *pair, w, f, out)


def store(lines, columns, payload_ref):
    rows = lines.shape[0]
    conts = lines.shape[1] // LANE
    for k in range(conts):
        payload_ref[k * rows:(k + 1) * rows, :] = lines[:, k * LANE:(k + 1) * LANE]
    if columns is not None:
        payload_ref[conts * rows:, :] = pack(columns)


def row_sum(value):
    return jnp.sum(value, axis=1, keepdims=True)


def flips(step, scen):
    return (step & (scen // 2 - 1)).bit_count() & 1


def half_of(s, b, scen, bits):
    s = s & (scen // 2 - 1)
    return sum((s >> i) + (b >> i) for i in range(bits)) & 1


def prepare_body(a_hbm, b_hbm, hess_hbm, high_ref, low_ref, mine_ref, theirs_ref, own_ref, extra_ref,
                 held_ref, b_ref, hess_ref, sems, *, scen, bits):
    conts = a_hbm.shape[0]
    copies = reads(a_hbm, held_ref, sems)
    first = pltpu.make_async_copy(b_hbm, b_ref, sems.at[conts])
    second = pltpu.make_async_copy(hess_hbm, hess_ref, sems.at[conts + 1])
    for copy in [first, second] + copies:
        copy.start()
    first.wait()
    second.wait()
    rows = b_ref.shape[0] // 2
    upper = half_of(lax.axis_index("scen"), lax.axis_index("base"), scen, bits) == 1
    low, high = b_ref[:rows, :], b_ref[rows:, :]
    own_ref[...] = jnp.where(upper, high, low)
    extra_ref[:rows, :] = jnp.where(upper, low, high)
    hess = hess_ref[...]
    extra_ref[rows:, :] = jnp.broadcast_to(hess, (8, hess.shape[1]))
    for k in range(conts):
        copies[k].wait()
        convert_one(k, held_ref, high_ref, low_ref)
    value = b_ref[...]
    lines = to_lines(value, high_ref, low_ref)
    sums = row_sum(value * value), row_sum(hess * value * value)

    def chosen(value, flip):
        one, two = (value[:rows], value[rows:]) if flip else (value[rows:], value[:rows])
        return jnp.where(upper, one, two)

    for flip, ref in ((False, mine_ref), (True, theirs_ref)):
        store(chosen(lines, flip), [chosen(value, flip) for value in sums], ref)


def summed(za_ref, zb_ref, rows, n):
    blocks = [za_ref[c * rows:(c + 1) * rows, :] + zb_ref[c * rows:(c + 1) * rows, :] for c in range(n // LANE)]
    return jnp.concatenate(blocks, axis=1)


def step_body(*refs, slot, first):
    with_slot(slot, refs[7:11], functools.partial(step_work, refs[:7], refs[11:], slot, first))


def step_work(ins, refs, slot, first, high_ref, low_ref):
    za_ref, zb_ref, r_ref, p_ref, x_ref, sc_ref, hess_ref = ins
    rows, n = r_ref.shape
    r = r_ref[...]
    hess = hess_ref[...]
    if slot == 0:
        out_ref, sums_ref, rn_ref, pn_ref, xn_ref, alpha_ref = refs
        top = n // LANE * rows
        curved = unpack(za_ref[top:, :] + zb_ref[top:, :], rows, 0)
        alpha = sc_ref[:, 0:1] / (curved + sc_ref[:, 1:2])
        alpha_ref[...] = jnp.broadcast_to(alpha, alpha_ref.shape)
    else:
        alpha_in, share_ref, share_sums, out_ref, rn_ref, pn_ref, xn_ref = refs
        alpha = alpha_in[:, 0:1]
    if first:
        p = r
        xn_ref[...] = alpha * p
    else:
        p = r + sc_ref[:, 2:3] * p_ref[...]
        xn_ref[...] = x_ref[...] + alpha * p
    pn_ref[...] = p
    r = r - alpha * (summed(za_ref, zb_ref, rows, n) + hess * p)
    rn_ref[...] = r
    scaled = hess * r
    columns = [row_sum(r * r), row_sum(scaled * r), row_sum(scaled * p)]
    sums = pack(columns)
    lines = to_lines(r, high_ref, low_ref)
    if slot == 0:
        sums_ref[...] = sums
        out_ref[...] = lines
    else:
        store(lines + share_ref[...], None, out_ref)
        out_ref[out_ref.shape[0] - 8:, :] = sums + share_sums[...]


def weigh(flows, k, w_ref, f_ref, out_ref):
    chosen = lane_index((1, LANE)) == out_ref[k:k + 1, :]
    factors = jnp.where(chosen, -1.0, f_ref[k:k + 1, :])
    hit = jnp.sum(jnp.where(chosen, flows, 0.0), axis=1, keepdims=True)
    post = flows + factors * hit
    return post, w_ref[k:k + 1, :] * post


def tree(refs, span):
    values = [ref[span, :] for ref in refs]
    if len(values) == 4:
        return (values[0] + values[3]) + (values[1] + values[2])
    return values[0] + values[1]


def lines_body(*refs, count, first, last):
    parts, refs = refs[:count], refs[count:]
    if last:
        lines_work(parts, refs[:7], refs[7:], first)
    else:
        with_slot(0, refs[7:11], functools.partial(lines_work, parts, refs[:7], refs[11:], first))


def lines_work(parts, ins, outs, first, *mats):
    fp_ref, fx_ref, sc_ref, alpha_ref, w_ref, f_ref, out_ref = ins
    last = not mats
    if last:
        z_ref, fpn_ref, fxn_ref, scn_ref = outs
    else:
        z_ref, pair_ref, fpn_ref, fxn_ref, scn_ref = outs
    conts = w_ref.shape[0]
    rows = parts[0].shape[0] // conts // 8 * 8

    def total(at, size):
        return tree(parts, slice(at, at + size))

    sums = total(conts * rows, 8)
    rr, base = unpack(sums, rows, 0), unpack(sums, rows, 1)
    if not first:
        beta = rr / sc_ref[:, 0:1]
        base = base + beta * (2.0 * unpack(sums, rows, 2) + beta * sc_ref[:, 1:2])
        alpha = alpha_ref[:, 0:1]
    lane = lane_index((rows, LANE))
    packed = jnp.where(lane == 0, rr, 0.0) + jnp.where(lane == 1, base, 0.0)
    if not first:
        packed = packed + jnp.where(lane == 2, beta, 0.0)
    scn_ref[...] = packed
    curv = jnp.zeros((rows, LANE), F32)
    flat = []
    for k in range(conts):
        span = slice(k * rows, (k + 1) * rows)
        flows = total(k * rows, rows)
        if not first:
            before = fp_ref[span, :]
            fxn_ref[span, :] = fx_ref[span, :] + alpha * before
            flows = flows + beta * before
        else:
            fxn_ref[span, :] = jnp.zeros((rows, LANE), F32)
        fpn_ref[span, :] = flows
        post, weighted = weigh(flows, k, w_ref, f_ref, out_ref)
        curv = curv + post * weighted
        flat.append(flows)
    curv = pack([row_sum(curv)])
    if last:
        z_ref[...] = curv
    else:
        pair = stacked(jnp.concatenate(flat, axis=1))
        pair_ref[...] = pair
        z_ref[z_ref.shape[0] - 8:, :] = curv
        from_lines(pair, z_ref, *mats)


def image_body(pair_ref, b0, b1, b2, b3, z_ref):
    with_slot(1, (b0, b1, b2, b3), functools.partial(from_lines, pair_ref[...], z_ref))


def finish_body(*refs, count):
    parts, refs = refs[:count], refs[count:]
    r0, r1, p0, p1, x0, x1, sc_ref, fp_ref, fx_ref, w_ref, f_ref, out_ref, own_ref, send_ref = refs
    rows, n = r0.shape
    alpha = sc_ref[:, 0:1] / (unpack(tree(parts, slice(None)), rows, 0) + sc_ref[:, 1:2])
    one, two = [x[...] + alpha * (r[...] + sc_ref[:, 2:3] * p[...]) for r, p, x in ((r0, p0, x0), (r1, p1, x1))]
    lower = core() == 0
    own_ref[:, :n] = jnp.where(lower, one, two)
    send_ref[:, :n] = jnp.where(lower, two, one)
    for k in range(w_ref.shape[0]):
        span = slice(k * rows, (k + 1) * rows)
        flows = fx_ref[span, :] + alpha * fp_ref[span, :]
        weighted = weigh(flows, k, w_ref, f_ref, out_ref)[1]
        own_ref[:, n + k * LANE:n + (k + 1) * LANE] = weighted
        send_ref[:, n + k * LANE:n + (k + 1) * LANE] = weighted


def place_body(own_ref, other_ref, part_ref, x_ref, w_ref):
    rows = own_ref.shape[0]
    n = x_ref.shape[1]
    upper = part_ref[0:1, 0:1] > 0
    for low in range(2):
        one, two = (other_ref, own_ref) if low == 0 else (own_ref, other_ref)
        value = jnp.where(upper, one[...], two[...])
        at = slice(low * rows, (low + 1) * rows)
        x_ref[at, :] = value[:, :n]
        for k in range(w_ref.shape[0]):
            w_ref[k, at, :] = value[:, n + k * LANE:n + (k + 1) * LANE]


def per_device(right_sides, base_hessian, sensitivity, weights, outage_factors, outaged, *, scen, base):
    conts, n, lines = sensitivity.shape
    rhs = right_sides.shape[0]
    rows = rhs // 2
    half = n // LANE * rows
    bits = max(scen, base).bit_length()
    spread = jnp.broadcast_to(outaged.astype(jnp.int32)[:, None], (conts, lines))

    def swap(value, *steps):
        pairs = []
        for s in range(scen):
            for b in range(base):
                along, across = steps[half_of(s, b, scen, bits) % len(steps)]
                pairs.append((s * base + b, (s ^ along) * base + (b ^ across)))
        return lax.ppermute(value, ("scen", "base"), pairs)

    def over_scen(value):
        bit = 2
        while 4 * bit < scen:
            value = value + swap(value, (bit | 1, 0))
            bit *= 2
        if 2 * bit < scen:
            one, two, both = (bit | 1, 0), (2 * bit, 0), (3 * bit | 1, 0)
            return [value, swap(value, both), swap(value, two), swap(value, one)]
        return [value, swap(value, (bit | 1, 0))]

    def over_base(values):
        order = [1 << i for i in range((base - 1).bit_length())]
        if len(values) == 1 and len(order) == 2:
            value, = values
            return [value, swap(value, (0, 3)), swap(value, (1, 2)), swap(value, (1, 1))]
        for i in range(len(order)):
            got = []
            for value in values:
                steps = [(1, order[(i + turn) % len(order)]) for turn in (0, 1)]
                got.append(swap(value, *steps))
            if i + 1 == len(order):
                return [v for both in zip(values, got) for v in both]
            values = [value + new for value, new in zip(values, got)]
            values[1:] = [lax.optimization_barrier((value, values[0]))[0] for value in values[1:]]

    part = half_of(lax.axis_index("scen"), lax.axis_index("base"), scen, bits)
    flat = struct((conts * rows, LANE))
    state = struct((rows, n))
    scal = struct((rows, LANE))
    payload = struct((conts * rows + 8, LANE))
    wide = [struct((half + 8, LANE)), struct((half, LANE))]
    share = struct((rows, conts * lines))
    pair = struct((2 * rows, conts * lines), BF16)
    block = struct((8, LANE))

    matrix = struct((n, conts * lines), BF16)
    high, low, mine, theirs, own, extra = pl.pallas_call(
        functools.partial(prepare_body, scen=scen, bits=bits),
        out_shape=[matrix, matrix, payload, payload, struct((rows, n)), struct((rows + 8, n))],
        in_specs=[pl.BlockSpec(memory_space=pltpu.HBM)] * 3,
        out_specs=[VM] * 6,
        scratch_shapes=[
            pltpu.VMEM(sensitivity.shape, F32),
            pltpu.VMEM(right_sides.shape, F32),
            pltpu.VMEM((1, n), F32),
            pltpu.SemaphoreType.DMA((conts + 2,)),
        ],
        compiler_params=PARAMS,
        name="prepare",
    )(*[pltpu.with_memory_space_constraint(v, pltpu.HBM) for v in (sensitivity, right_sides, base_hessian.reshape(1, n))])
    pay = mine + swap(theirs, (1, 0))
    held, late, pay = lax.optimization_barrier((sensitivity, extra, pay))
    other_a = swap(held, (1, 0))
    other = swap(late, (1, 0))
    lower = core() == 0

    def by_core(one, two):
        return [jnp.where(lower, one, two), jnp.where(lower, two, one)]

    r = by_core(own, other[:rows])
    hess = by_core(base_hessian[None, :], other[rows:rows + 1])
    table = (weights, outage_factors, spread)
    turned = struct((conts * lines, n), BF16)
    absorbed = pl.pallas_call(
        absorb_body,
        out_shape=[turned, turned, matrix, matrix, turned, turned],
        in_specs=[pl.BlockSpec(memory_space=pltpu.HBM)] + [VM] * 5,
        out_specs=[VM] * 6,
        scratch_shapes=[pltpu.VMEM(sensitivity.shape, F32), pltpu.SemaphoreType.DMA((conts,))],
        compiler_params=PARAMS,
        name="absorb",
    )(pltpu.with_memory_space_constraint(other_a, pltpu.HBM), high, low, *table)
    mats = [high, low, *absorbed[2:4]]
    folded = [*absorbed[:2], *absorbed[4:]]
    p, x = list(r), list(r)
    fp = fx = jnp.zeros(flat.shape, F32)
    sc = alpha = jnp.zeros(scal.shape, F32)
    for it in range(ITERS):
        first, last = it == 0, it + 1 == ITERS
        sent = over_scen(pay)
        got = call(
            functools.partial(lines_body, count=len(sent), first=first, last=last),
            [*([block] if last else [wide[0], pair]), flat, flat, scal], "lines",
            *sent, fp, fx, sc, alpha, *table, *(() if last else folded))
        fp, fx, sc = got[-3:]
        if last:
            z = over_base(got[:1])
            break
        z = over_base([got[0], call(image_body, wide[1], "image", got[1], *folded)])
        share_lines, share_sums, r[0], p[0], x[0], alpha = call(
            functools.partial(step_body, slot=0, first=first),
            [share, block, state, state, state, scal], "step",
            *z[:2], r[0], p[0], x[0], sc, hess[0], *mats)
        pay, r[1], p[1], x[1] = call(
            functools.partial(step_body, slot=1, first=first),
            [payload, state, state, state], "step",
            *z[2:], r[1], p[1], x[1], sc, hess[1], *mats, alpha, share_lines, share_sums)
    both = struct((rows, n + conts * LANE))
    own, send = call(functools.partial(finish_body, count=len(z)), [both, both], "finish", *z, *r, *p, *x, sc, fp, fx, *table)
    recv = swap(send, (1, 0))
    which = jnp.broadcast_to(part.astype(jnp.int32), (8, LANE))
    step, flow = call(place_body, [struct((rhs, n)), struct((conts, rhs, lines))], "place", own, recv, which)
    return step, flow


def solution(mesh):
    placed = (
        P(None, "scen"),
        P("scen"),
        P("base", "scen", None),
        P("base", None),
        P("base", None),
        P("base"),
    )
    body = functools.partial(per_device, scen=mesh.shape["scen"], base=mesh.shape["base"])
    return jax.shard_map(
        body,
        mesh=mesh,
        in_specs=placed,
        out_specs=(P(None, "scen"), P("base", None, None)),
        check_vma=False,
    )
```

```python
import functools

import jax
import jax.numpy as jnp
from jax import lax
from jax.experimental import pallas as pl
from jax.experimental.pallas import tpu as pltpu
from jax.sharding import PartitionSpec as P

ITERS = 5
LANE = 128
F32 = jnp.float32
BF16 = jnp.bfloat16
VM = pl.BlockSpec(memory_space=pltpu.VMEM)
PARAMS = pltpu.CompilerParams(vmem_limit_bytes=24 * 1024 * 1024)


def call(body, out_shape, name, *args):
    many = isinstance(out_shape, (list, tuple))
    return pl.pallas_call(
        body,
        out_shape=out_shape,
        in_specs=[VM] * len(args),
        out_specs=[VM] * len(out_shape) if many else VM,
        compiler_params=PARAMS,
        name=name,
    )(*args)


def struct(shape, dtype=F32):
    return jax.ShapeDtypeStruct(shape, dtype)


def split(value):
    high = value.astype(BF16)
    low = (value - high.astype(F32)).astype(BF16)
    return high, low


def stacked(value):
    high, low = split(value)
    return jnp.concatenate([high, low], axis=0)


def lane_index(shape):
    return lax.broadcasted_iota(jnp.int32, shape, 1)


def pack(columns):
    lane = lane_index((8, LANE))
    block = jnp.zeros((8, LANE), F32)
    at = 0
    for column in columns:
        for row in range(0, column.shape[0], 8):
            block = jnp.where(lane == at, column[row:row + 8], block)
            at += 1
    return block


def unpack(block, rows, index):
    groups = rows // 8
    return jnp.concatenate([block[:, index * groups + g:index * groups + g + 1] for g in range(groups)], axis=0)


def core():
    return lax.axis_index("scen") & 1


def with_slot(slot, refs, body):
    own = core() == slot

    @pl.when(own)
    def _():
        body(*refs[:2])

    @pl.when(jnp.logical_not(own))
    def _():
        body(*refs[2:])


def dot(lhs, rhs, rhs_dim):
    return lax.dot_general(lhs, rhs, (((1,), (rhs_dim,)), ((), ())), preferred_element_type=F32)


def to_lines(vector, high_ref, low_ref):
    rows = vector.shape[0]
    pair = stacked(vector)
    main, rest = dot(pair, high_ref[...], 0), dot(pair[:rows], low_ref[...], 0)
    return main[:rows] + (main[rows:] + rest)


def from_lines(pair, z_ref, high_ref, low_ref):
    rows = pair.shape[0] // 2
    main, rest = dot(pair, high_ref[...], 0), dot(pair[:rows], low_ref[...], 0)
    image = main[:rows] + (main[rows:] + rest)
    for c in range(image.shape[1] // LANE):
        z_ref[c * rows:(c + 1) * rows, :] = image[:, c * LANE:(c + 1) * LANE]


def operator(w, f, out):
    row = lax.broadcasted_iota(jnp.int32, (LANE, LANE), 0)
    col = lax.broadcasted_iota(jnp.int32, (LANE, LANE), 1)
    lane = lane_index((1, LANE))
    kept = jnp.where(lane == out, 0.0, f)
    gain = w * kept
    corner = jnp.sum(gain * kept, axis=1, keepdims=True)
    edge = jnp.where(row == out, gain, 0.0)
    inner = jnp.where(row == col, jnp.where(col == out, corner, w), 0.0)
    return inner + edge + edge.T


def fold_one(k, high_ref, low_ref, w_ref, f_ref, out_ref, bh_ref, bl_ref):
    span = slice(k * LANE, (k + 1) * LANE)
    op = operator(w_ref[k:k + 1, :], f_ref[k:k + 1, :], out_ref[k:k + 1, :])
    pair = stacked(op)
    main = dot(pair, high_ref[:, span], 1)
    rest = dot(pair[:LANE], low_ref[:, span], 1)
    high, low = split(main[:LANE] + (main[LANE:] + rest))
    bh_ref[span, :] = high
    bl_ref[span, :] = low


def fold_body(high_ref, low_ref, w_ref, f_ref, out_ref, bh_ref, bl_ref):
    for k in range(w_ref.shape[0]):
        fold_one(k, high_ref, low_ref, w_ref, f_ref, out_ref, bh_ref, bl_ref)


def reads(a_hbm, held_ref, sems):
    return [pltpu.make_async_copy(a_hbm.at[k], held_ref.at[k], sems.at[k]) for k in range(a_hbm.shape[0])]


def convert_one(k, held_ref, high_ref, low_ref):
    high, low = split(held_ref[k])
    high_ref[:, k * LANE:(k + 1) * LANE] = high
    low_ref[:, k * LANE:(k + 1) * LANE] = low


def absorb_body(a_hbm, own_high, own_low, w_ref, f_ref, out_ref, oh_ref, ol_ref,
                high_ref, low_ref, bh_ref, bl_ref, held_ref, sems):
    copies = reads(a_hbm, held_ref, sems)
    for copy in copies:
        copy.start()
    for k in range(len(copies)):
        fold_one(k, own_high, own_low, w_ref, f_ref, out_ref, oh_ref, ol_ref)
    for k, copy in enumerate(copies):
        copy.wait()
        convert_one(k, held_ref, high_ref, low_ref)
        fold_one(k, high_ref, low_ref, w_ref, f_ref, out_ref, bh_ref, bl_ref)


def fold(pair, w, f, out):
    n, m = pair[0].shape
    shape = struct((m, n), BF16)
    return call(fold_body, [shape, shape], "fold", *pair, w, f, out)


def store(lines, columns, payload_ref):
    rows = lines.shape[0]
    conts = lines.shape[1] // LANE
    for k in range(conts):
        payload_ref[k * rows:(k + 1) * rows, :] = lines[:, k * LANE:(k + 1) * LANE]
    if columns is not None:
        payload_ref[conts * rows:, :] = pack(columns)


def row_sum(value):
    return jnp.sum(value, axis=1, keepdims=True)


def flips(step, scen):
    return (step & (scen // 2 - 1)).bit_count() & 1


def half_of(s, b, scen, bits):
    s = s & (scen // 2 - 1)
    return sum((s >> i) + (b >> i) for i in range(bits)) & 1


def prepare_body(a_hbm, b_hbm, hess_hbm, high_ref, low_ref, mine_ref, theirs_ref, own_ref, extra_ref,
                 held_ref, b_ref, hess_ref, sems, *, scen, bits):
    conts = a_hbm.shape[0]
    copies = reads(a_hbm, held_ref, sems)
    first = pltpu.make_async_copy(b_hbm, b_ref, sems.at[conts])
    second = pltpu.make_async_copy(hess_hbm, hess_ref, sems.at[conts + 1])
    for copy in [first, second] + copies:
        copy.start()
    first.wait()
    second.wait()
    rows = b_ref.shape[0] // 2
    upper = half_of(lax.axis_index("scen"), lax.axis_index("base"), scen, bits) == 1
    low, high = b_ref[:rows, :], b_ref[rows:, :]
    own_ref[...] = jnp.where(upper, high, low)
    extra_ref[:rows, :] = jnp.where(upper, low, high)
    hess = hess_ref[...]
    extra_ref[rows:, :] = jnp.broadcast_to(hess, (8, hess.shape[1]))
    for k in range(conts):
        copies[k].wait()
        convert_one(k, held_ref, high_ref, low_ref)
    value = b_ref[...]
    lines = to_lines(value, high_ref, low_ref)
    sums = row_sum(value * value), row_sum(hess * value * value)

    def chosen(value, flip):
        one, two = (value[:rows], value[rows:]) if flip else (value[rows:], value[:rows])
        return jnp.where(upper, one, two)

    for flip, ref in ((False, mine_ref), (True, theirs_ref)):
        store(chosen(lines, flip), [chosen(value, flip) for value in sums], ref)


def summed(za_ref, zb_ref, rows, n):
    blocks = [za_ref[c * rows:(c + 1) * rows, :] + zb_ref[c * rows:(c + 1) * rows, :] for c in range(n // LANE)]
    return jnp.concatenate(blocks, axis=1)


def step_body(*refs, slot, first):
    with_slot(slot, refs[7:11], functools.partial(step_work, refs[:7], refs[11:], slot, first))


def step_work(ins, refs, slot, first, high_ref, low_ref):
    za_ref, zb_ref, r_ref, p_ref, x_ref, sc_ref, hess_ref = ins
    rows, n = r_ref.shape
    r = r_ref[...]
    hess = hess_ref[...]
    if slot == 0:
        out_ref, sums_ref, rn_ref, pn_ref, xn_ref, alpha_ref = refs
        top = n // LANE * rows
        curved = unpack(za_ref[top:, :] + zb_ref[top:, :], rows, 0)
        alpha = sc_ref[:, 0:1] / (curved + sc_ref[:, 1:2])
        alpha_ref[...] = jnp.broadcast_to(alpha, alpha_ref.shape)
    else:
        alpha_in, share_ref, share_sums, out_ref, rn_ref, pn_ref, xn_ref = refs
        alpha = alpha_in[:, 0:1]
    if first:
        p = r
        xn_ref[...] = alpha * p
    else:
        p = r + sc_ref[:, 2:3] * p_ref[...]
        xn_ref[...] = x_ref[...] + alpha * p
    pn_ref[...] = p
    r = r - alpha * (summed(za_ref, zb_ref, rows, n) + hess * p)
    rn_ref[...] = r
    scaled = hess * r
    columns = [row_sum(r * r), row_sum(scaled * r), row_sum(scaled * p)]
    sums = pack(columns)
    lines = to_lines(r, high_ref, low_ref)
    if slot == 0:
        sums_ref[...] = sums
        out_ref[...] = lines
    else:
        store(lines + share_ref[...], None, out_ref)
        out_ref[out_ref.shape[0] - 8:, :] = sums + share_sums[...]


def weigh(flows, k, w_ref, f_ref, out_ref):
    chosen = lane_index((1, LANE)) == out_ref[k:k + 1, :]
    factors = jnp.where(chosen, -1.0, f_ref[k:k + 1, :])
    hit = jnp.sum(jnp.where(chosen, flows, 0.0), axis=1, keepdims=True)
    post = flows + factors * hit
    return post, w_ref[k:k + 1, :] * post


def tree(refs, span):
    values = [ref[span, :] for ref in refs]
    if len(values) == 4:
        return (values[0] + values[3]) + (values[1] + values[2])
    return values[0] + values[1]


def lines_body(*refs, count, first, last):
    parts, refs = refs[:count], refs[count:]
    if last:
        lines_work(parts, refs[:7], refs[7:], first)
    else:
        with_slot(0, refs[7:11], functools.partial(lines_work, parts, refs[:7], refs[11:], first))


def lines_work(parts, ins, outs, first, *mats):
    fp_ref, fx_ref, sc_ref, alpha_ref, w_ref, f_ref, out_ref = ins
    last = not mats
    if last:
        z_ref, fpn_ref, fxn_ref, scn_ref = outs
    else:
        z_ref, pair_ref, fpn_ref, fxn_ref, scn_ref = outs
    conts = w_ref.shape[0]
    rows = parts[0].shape[0] // conts // 8 * 8

    def total(at, size):
        return tree(parts, slice(at, at + size))

    sums = total(conts * rows, 8)
    rr, base = unpack(sums, rows, 0), unpack(sums, rows, 1)
    if not first:
        beta = rr / sc_ref[:, 0:1]
        base = base + beta * (2.0 * unpack(sums, rows, 2) + beta * sc_ref[:, 1:2])
        alpha = alpha_ref[:, 0:1]
    lane = lane_index((rows, LANE))
    packed = jnp.where(lane == 0, rr, 0.0) + jnp.where(lane == 1, base, 0.0)
    if not first:
        packed = packed + jnp.where(lane == 2, beta, 0.0)
    scn_ref[...] = packed
    curv = jnp.zeros((rows, LANE), F32)
    flat = []
    for k in range(conts):
        span = slice(k * rows, (k + 1) * rows)
        flows = total(k * rows, rows)
        if not first:
            before = fp_ref[span, :]
            fxn_ref[span, :] = fx_ref[span, :] + alpha * before
            flows = flows + beta * before
        else:
            fxn_ref[span, :] = jnp.zeros((rows, LANE), F32)
        fpn_ref[span, :] = flows
        post, weighted = weigh(flows, k, w_ref, f_ref, out_ref)
        curv = curv + post * weighted
        flat.append(flows)
    curv = pack([row_sum(curv)])
    if last:
        z_ref[...] = curv
    else:
        pair = stacked(jnp.concatenate(flat, axis=1))
        pair_ref[...] = pair
        z_ref[z_ref.shape[0] - 8:, :] = curv
        from_lines(pair, z_ref, *mats)


def image_body(pair_ref, b0, b1, b2, b3, z_ref):
    with_slot(1, (b0, b1, b2, b3), functools.partial(from_lines, pair_ref[...], z_ref))


def finish_body(*refs, count):
    parts, refs = refs[:count], refs[count:]
    r0, r1, p0, p1, x0, x1, sc_ref, fp_ref, fx_ref, w_ref, f_ref, out_ref, own_ref, send_ref = refs
    rows, n = r0.shape
    alpha = sc_ref[:, 0:1] / (unpack(tree(parts, slice(None)), rows, 0) + sc_ref[:, 1:2])
    one, two = [x[...] + alpha * (r[...] + sc_ref[:, 2:3] * p[...]) for r, p, x in ((r0, p0, x0), (r1, p1, x1))]
    lower = core() == 0
    own_ref[:, :n] = jnp.where(lower, one, two)
    send_ref[:, :n] = jnp.where(lower, two, one)
    for k in range(w_ref.shape[0]):
        span = slice(k * rows, (k + 1) * rows)
        flows = fx_ref[span, :] + alpha * fp_ref[span, :]
        weighted = weigh(flows, k, w_ref, f_ref, out_ref)[1]
        own_ref[:, n + k * LANE:n + (k + 1) * LANE] = weighted
        send_ref[:, n + k * LANE:n + (k + 1) * LANE] = weighted


def place_body(own_ref, other_ref, part_ref, x_ref, w_ref):
    rows = own_ref.shape[0]
    n = x_ref.shape[1]
    upper = part_ref[0:1, 0:1] > 0
    for low in range(2):
        one, two = (other_ref, own_ref) if low == 0 else (own_ref, other_ref)
        value = jnp.where(upper, one[...], two[...])
        at = slice(low * rows, (low + 1) * rows)
        x_ref[at, :] = value[:, :n]
        for k in range(w_ref.shape[0]):
            w_ref[k, at, :] = value[:, n + k * LANE:n + (k + 1) * LANE]


def per_device(right_sides, base_hessian, sensitivity, weights, outage_factors, outaged, *, scen, base):
    conts, n, lines = sensitivity.shape
    rhs = right_sides.shape[0]
    rows = rhs // 2
    half = n // LANE * rows
    bits = max(scen, base).bit_length()
    spread = jnp.broadcast_to(outaged.astype(jnp.int32)[:, None], (conts, lines))

    def swap(value, *steps):
        pairs = []
        for s in range(scen):
            for b in range(base):
                along, across = steps[half_of(s, b, scen, bits) % len(steps)]
                pairs.append((s * base + b, (s ^ along) * base + (b ^ across)))
        return lax.ppermute(value, ("scen", "base"), pairs)

    def over_scen(value):
        bit = 2
        while 4 * bit < scen:
            value = value + swap(value, (bit | 1, 0))
            bit *= 2
        if 2 * bit < scen:
            one, two, both = (bit | 1, 0), (2 * bit, 0), (3 * bit | 1, 0)
            return [value, swap(value, both), swap(value, two), swap(value, one)]
        return [value, swap(value, (bit | 1, 0))]

    def over_base(values):
        order = [1 << i for i in range((base - 1).bit_length())]
        if len(values) == 1 and len(order) == 2:
            value, = values
            return [value, swap(value, (0, 3)), swap(value, (1, 2)), swap(value, (1, 1))]
        for i in range(len(order)):
            got = []
            for value in values:
                steps = [(1, order[(i + turn) % len(order)]) for turn in (0, 1)]
                got.append(swap(value, *steps))
            if i + 1 == len(order):
                return [v for both in zip(values, got) for v in both]
            values = [value + new for value, new in zip(values, got)]
            values[1:] = [lax.optimization_barrier((value, values[0]))[0] for value in values[1:]]

    part = half_of(lax.axis_index("scen"), lax.axis_index("base"), scen, bits)
    flat = struct((conts * rows, LANE))
    state = struct((rows, n))
    scal = struct((rows, LANE))
    payload = struct((conts * rows + 8, LANE))
    wide = [struct((half + 8, LANE)), struct((half, LANE))]
    share = struct((rows, conts * lines))
    pair = struct((2 * rows, conts * lines), BF16)
    block = struct((8, LANE))

    matrix = struct((n, conts * lines), BF16)
    high, low, mine, theirs, own, extra = pl.pallas_call(
        functools.partial(prepare_body, scen=scen, bits=bits),
        out_shape=[matrix, matrix, payload, payload, struct((rows, n)), struct((rows + 8, n))],
        in_specs=[pl.BlockSpec(memory_space=pltpu.HBM)] * 3,
        out_specs=[VM] * 6,
        scratch_shapes=[
            pltpu.VMEM(sensitivity.shape, F32),
            pltpu.VMEM(right_sides.shape, F32),
            pltpu.VMEM((1, n), F32),
            pltpu.SemaphoreType.DMA((conts + 2,)),
        ],
        compiler_params=PARAMS,
        name="prepare",
    )(*[pltpu.with_memory_space_constraint(v, pltpu.HBM) for v in (sensitivity, right_sides, base_hessian.reshape(1, n))])
    pay = mine + swap(theirs, (1, 0))
    held, late, pay = lax.optimization_barrier((sensitivity, extra, pay))
    other_a = swap(held, (1, 0))
    other = swap(late, (1, 0))
    lower = core() == 0

    def by_core(one, two):
        return [jnp.where(lower, one, two), jnp.where(lower, two, one)]

    r = by_core(own, other[:rows])
    hess = by_core(base_hessian[None, :], other[rows:rows + 1])
    table = (weights, outage_factors, spread)
    turned = struct((conts * lines, n), BF16)
    absorbed = pl.pallas_call(
        absorb_body,
        out_shape=[turned, turned, matrix, matrix, turned, turned],
        in_specs=[pl.BlockSpec(memory_space=pltpu.HBM)] + [VM] * 5,
        out_specs=[VM] * 6,
        scratch_shapes=[pltpu.VMEM(sensitivity.shape, F32), pltpu.SemaphoreType.DMA((conts,))],
        compiler_params=PARAMS,
        name="absorb",
    )(pltpu.with_memory_space_constraint(other_a, pltpu.HBM), high, low, *table)
    mats = [high, low, *absorbed[2:4]]
    folded = [*absorbed[:2], *absorbed[4:]]
    p, x = list(r), list(r)
    fp = fx = jnp.zeros(flat.shape, F32)
    sc = alpha = jnp.zeros(scal.shape, F32)
    for it in range(ITERS):
        first, last = it == 0, it + 1 == ITERS
        sent = over_scen(pay)
        got = call(
            functools.partial(lines_body, count=len(sent), first=first, last=last),
            [*([block] if last else [wide[0], pair]), flat, flat, scal], "lines",
            *sent, fp, fx, sc, alpha, *table, *(() if last else folded))
        fp, fx, sc = got[-3:]
        if last:
            z = over_base(got[:1])
            break
        z = over_base([got[0], call(image_body, wide[1], "image", got[1], *folded)])
        share_lines, share_sums, r[0], p[0], x[0], alpha = call(
            functools.partial(step_body, slot=0, first=first),
            [share, block, state, state, state, scal], "step",
            *z[:2], r[0], p[0], x[0], sc, hess[0], *mats)
        pay, r[1], p[1], x[1] = call(
            functools.partial(step_body, slot=1, first=first),
            [payload, state, state, state], "step",
            *z[2:], r[1], p[1], x[1], sc, hess[1], *mats, alpha, share_lines, share_sums)
    both = struct((rows, n + conts * LANE))
    own, send = call(functools.partial(finish_body, count=len(z)), [both, both], "finish", *z, *r, *p, *x, sc, fp, fx, *table)
    recv = swap(send, (1, 0))
    which = jnp.broadcast_to(part.astype(jnp.int32), (8, LANE))
    step, flow = call(place_body, [struct((rhs, n)), struct((conts, rhs, lines))], "place", own, recv, which)
    return step, flow


def solution(mesh):
    placed = (
        P(None, "scen"),
        P("scen"),
        P("base", "scen", None),
        P("base", None),
        P("base", None),
        P("base"),
    )
    body = functools.partial(per_device, scen=mesh.shape["scen"], base=mesh.shape["base"])
    return jax.shard_map(
        body,
        mesh=mesh,
        in_specs=placed,
        out_specs=(P(None, "scen"), P("base", None, None)),
        check_vma=False,
    )
```
